8 devices in a mesh: data: 1 (over z), col: 2 (over y), row: 4 (over x, core).
Axes of the slice: x: 2, y: 2, z: 1, core: 2. Of those that a mesh axis runs over, the one named last changes fastest.
Arguments:
- residual: bfloat16 [256, 4096], P('data', 'row')
- gain_mlp: float32 [4096], P('row')
- gain_attn: float32 [4096], P('row')
- w_gate: bfloat16 [4096, 11008], P(None, ('col', 'row'))
- w_up: bfloat16 [4096, 11008], P(None, ('col', 'row'))
- w_down: bfloat16 [11008, 4096], P('col', 'row')
- w_qkv: bfloat16 [4096, 12288], P(None, ('col', 'row'))
Outputs:
- output 1: bfloat16 [256, 4096], P('data', 'row')
- output 2: bfloat16 [256, 12288], P('data', ('col', 'row'))
All inputs are finite; a program needn't handle non-finite values.
Results may differ from the reference program's by a relative error of at most 0.00403686.
Values are sent between devices in bfloat16 or wider.
A program may use at most 1 GiB of HBM per device.

```python
import math
import jax
import jax.numpy as jnp
from jax import lax

TOKENS = 256
D = 4096
FF = 11008
HEADS = 32
KV_HEADS = 32
HEAD_DIM = 128
QKV_WIDTH = (HEADS + 2 * KV_HEADS) * HEAD_DIM
NORM_EPS = 1e-6


def setup_inputs(seed: int = 0, part: int = 0) -> dict:
    key_list = jax.random.split(jax.random.key(seed), 8)
    tok_keys = jax.random.split(jax.random.fold_in(key_list[0], part), 3)
    base_vals = jax.random.normal(tok_keys[0], (TOKENS, D), jnp.float32)
    tok_scale = jnp.exp(jax.random.uniform(tok_keys[1], (TOKENS, 1), jnp.float32, -1.0, 1.0))
    wave_amps = jax.random.normal(tok_keys[2], (TOKENS, 2), jnp.float32)
    angles = jnp.arange(D, dtype=jnp.float32) * (2.0 * math.pi / D)
    profile = jnp.exp(0.7 * (wave_amps[:, 0:1] * jnp.cos(angles) + wave_amps[:, 1:2] * jnp.sin(angles)))
    residual = (base_vals * tok_scale * profile).astype(jnp.bfloat16)
    gain_mlp = jax.random.uniform(key_list[1], (D,), jnp.float32, 0.4, 1.6)
    gain_attn = jax.random.uniform(key_list[2], (D,), jnp.float32, 0.4, 1.6)
    w_gate = (jax.random.normal(key_list[3], (D, FF), jnp.float32) * D ** -0.5).astype(jnp.bfloat16)
    w_up = (jax.random.normal(key_list[4], (D, FF), jnp.float32) * D ** -0.5).astype(jnp.bfloat16)
    w_down = (jax.random.normal(key_list[5], (FF, D), jnp.float32) * FF ** -0.5).astype(jnp.bfloat16)
    w_qkv = (jax.random.normal(key_list[6], (D, QKV_WIDTH), jnp.float32) * D ** -0.5).astype(jnp.bfloat16)
    return {'residual': residual, 'gain_mlp': gain_mlp, 'gain_attn': gain_attn, 'w_gate': w_gate, 'w_up': w_up, 'w_down': w_down, 'w_qkv': w_qkv}


def rms_normed(rows, gain):
    rows_f = rows.astype(jnp.float32)
    row_scale = lax.rsqrt(jnp.mean(rows_f * rows_f, axis=1, keepdims=True) + NORM_EPS)
    return (rows_f * row_scale * gain).astype(jnp.bfloat16)


def reference(residual, gain_mlp, gain_attn, w_gate, w_up, w_down, w_qkv):
    normed = rms_normed(residual, gain_mlp)
    gate_val = jnp.dot(normed, w_gate, preferred_element_type=jnp.float32)
    up_val = jnp.dot(normed, w_up, preferred_element_type=jnp.float32)
    act_val = (jax.nn.silu(gate_val) * up_val).astype(jnp.bfloat16)
    down_val = jnp.dot(act_val, w_down, preferred_element_type=jnp.float32)
    resid_next = (residual.astype(jnp.float32) + down_val).astype(jnp.bfloat16)
    normed_next = rms_normed(resid_next, gain_attn)
    qkv_out = jnp.dot(normed_next, w_qkv, preferred_element_type=jnp.float32).astype(jnp.bfloat16)
    return (resid_next, qkv_out)
```

```python
import functools

import jax
import jax.numpy as jnp
from jax import lax
from jax.experimental import pallas as pl
from jax.experimental.pallas import tpu as pltpu
from jax.sharding import PartitionSpec as P

NORM_EPS = 1e-6
MESH = pl.DeviceIdType.MESH
F32, BF16 = jnp.float32, jnp.bfloat16

X_PIECES = 4
GROUPS = ((0, 256), (256, 512), (768, 608))
CHUNKS = ((0, 64), (64, 64), (128, 64), (192, 64))
SENDS = (((0, 0), (0, 1), (0, 2), (0, 3)),
         ((1, 0), (1, 1)),
         ((2, 0), (2, 1), (1, 2), (2, 2), (1, 3), (2, 3)))
ORDER = tuple(b for s in SENDS for b in s)
W_PARTS = 8


def dot_t(a, b):
    return lax.dot_general(a, b, (((1,), (1,)), ((), ())), preferred_element_type=F32)


class Names:
    def __init__(self):
        self.table = {}

    def __call__(self, *key):
        return self.table.setdefault(key, len(self.table))


def kernel(tokens, width, ff, names, local_names,
           x_hbm, g1_hbm, g2_hbm, wg_hbm, wu_hbm, wd_hbm, wq_hbm, res_hbm, qkv_hbm,
           xg, nb, wg, wu, wd, wq, ag, acc, rbuf, xn, g1, g2, out, send_sem, recv_sem, loc_sem):
    data, y, row = lax.axis_index("data"), lax.axis_index("col"), lax.axis_index("row")
    cx = row // 2
    core = row - cx * 2
    sib_row = cx * 2 + 1 - core
    far_row = (1 - cx) * 2 + core
    fsib_row = (1 - cx) * 2 + 1 - core
    sib, far, fsib = (data, y, sib_row), (data, y, far_row), (data, y, fsib_row)
    up, diag = (data, 1 - y, row), (data, 1 - y, far_row)
    hidden = width * 4
    half = tokens // 2

    def remote(key, src, dst, dev):
        i = names(*key)
        return pltpu.make_async_remote_copy(src_ref=src, dst_ref=dst, send_sem=send_sem.at[i], recv_sem=recv_sem.at[i],
                                            device_id=dev, device_id_type=MESH)

    def local(key, src, dst):
        return pltpu.make_async_copy(src, dst, loc_sem.at[local_names(*key)])

    sent = []

    def go(copy):
        copy.start()
        sent.append(copy)
        return copy

    own = [local(("x",), x_hbm, xg.at[row]), local(("g1",), g1_hbm, g1.at[row]), local(("g2",), g2_hbm, g2.at[row])]
    for c in own:
        c.start()
    loads = {}
    for name, src, dst in (("wg", wg_hbm, wg), ("wu", wu_hbm, wu)):
        loads[name] = [local((name, i), src.at[pl.ds(c0, cn)], dst.at[pl.ds(c0, cn)]) for i, (c0, cn) in enumerate(GROUPS)]
    loads["wd"] = [local(("wd", i), wd_hbm.at[pl.ds(i * ff, ff)], wd.at[i]) for i in range(4)]
    part = hidden // W_PARTS
    loads["wq"] = [local(("wq", i), wq_hbm.at[pl.ds(i * part, part)], wq.at[pl.ds(i * part, part)]) for i in range(W_PARTS)]
    for pair in zip(loads["wg"], loads["wu"]):
        for c in pair:
            c.start()
    for name in ("wd", "wq"):
        for c in loads[name]:
            c.start()

    barrier = pltpu.get_barrier_semaphore()
    for dev in (sib, far, fsib, up, diag):
        pl.semaphore_signal(barrier, inc=1, device_id=dev, device_id_type=MESH)
    pl.semaphore_wait(barrier, 5)

    for c in own:
        c.wait()
    piece = half // X_PIECES

    def rows_of(side, p):
        return pl.ds(pl.multiple_of(side * half + p * piece, piece), piece)

    gains = []
    for tag, dev in (("s", sib), ("f", far), ("fs", fsib)):
        for name, ref in (("g1", g1), ("g2", g2)):
            gains.append(go(remote((name, tag), ref.at[row], ref.at[row], dev)))
    x_far = [go(remote(("xx", p), xg.at[row, rows_of(y, p)], xg.at[row, rows_of(y, p)], far)) for p in range(X_PIECES)]
    x_sib = go(remote(("xs",), xg.at[row], xg.at[row], sib))

    def norm(src, gain, rows0, count):
        def step(i, carry):
            rows = pl.ds(pl.multiple_of(rows0 + i * 16, 16), 16)
            blocks = [src[b, rows].astype(F32) for b in range(4)]
            total = sum(jnp.sum(v * v, axis=1, keepdims=True) for v in blocks)
            scale = lax.rsqrt(total / hidden + NORM_EPS)
            for b in range(4):
                nb[rows, b * width:(b + 1) * width] = (blocks[b] * scale * gain[b]).astype(BF16)
            return carry
        lax.fori_loop(0, count // 16, step, 0)

    x_up, x_fs = [], []

    def ready_direct(p):
        x_far[p].wait_recv()
        blk = xg.at[far_row, rows_of(y, p)]
        x_up.append(go(remote(("xy", p), blk, blk, up)))
        x_fs.append(go(remote(("xf", p), blk, blk, sib)))

    def ready_relayed(p):
        x_up[p].wait_recv()
        blk = xg.at[far_row, rows_of(1 - y, p)]
        x_fs.append(go(remote(("xf", X_PIECES + p), blk, blk, sib)))

    def norm_piece(q):
        x_fs[q].wait_recv()
        side, p = (y, q) if q < X_PIECES else (1 - y, q - X_PIECES)
        norm(xg, g1, side * half + p * piece, piece)

    for p in range(X_PIECES):
        ready_direct(p)
        if p == 0:
            for c in gains:
                c.wait_recv()
            x_sib.wait_recv()
        else:
            norm_piece(p - 1)
    for p in range(X_PIECES):
        ready_relayed(p)
        norm_piece(X_PIECES + p - 1)
    norm_piece(2 * X_PIECES - 1)

    a_sib, a_far, a_fs = {}, {}, {}
    for g, (c0, cn) in enumerate(GROUPS):
        cols = slice(c0, c0 + cn)
        loads["wg"][g].wait()
        loads["wu"][g].wait()
        gate = dot_t(wg[cols], nb[...])
        upv = dot_t(wu[cols], nb[...])
        ag[row, :, cols] = (jax.nn.silu(gate) * upv).astype(BF16).T
        for (gg, t) in SENDS[g]:
            t0, tn = CHUNKS[t]
            b0, bn = GROUPS[gg]
            blk = ag.at[row, pl.ds(t0, tn), pl.ds(b0, bn)]
            a_far[gg, t] = go(remote(("ax", gg, t), blk, blk, far))
        blk = ag.at[row, :, pl.ds(c0, cn)]
        a_sib[g] = go(remote(("as", g), blk, blk, sib))

    def forward(gg, t):
        a_far[gg, t].wait_recv()
        t0, tn = CHUNKS[t]
        b0, bn = GROUPS[gg]
        blk = ag.at[far_row, pl.ds(t0, tn), pl.ds(b0, bn)]
        a_fs[gg, t] = go(remote(("af", gg, t), blk, blk, sib))

    queue = list(ORDER)
    for _ in range(4):
        forward(*queue.pop(0))
    for c in loads["wd"]:
        c.wait()
    acc[...] = jnp.dot(ag[row], wd[row], preferred_element_type=F32)
    forward(*queue.pop(0))
    for c in a_sib.values():
        c.wait_recv()
    acc[...] += jnp.dot(ag[sib_row], wd[sib_row], preferred_element_type=F32)

    rs, xp, xf = {}, {}, {}

    def down(t):
        t0, tn = CHUNKS[t]
        need = max(queue.index(b) for b in queue if b[1] == t) if any(b[1] == t for b in queue) else -1
        for _ in range(need + 1):
            forward(*queue.pop(0))
        rows = slice(t0, t0 + tn)
        acc[rows] += jnp.dot(ag[far_row, rows], wd[far_row], preferred_element_type=F32)
        for g in range(len(GROUPS)):
            a_fs[g, t].wait_recv()
        acc[rows] += jnp.dot(ag[fsib_row, rows], wd[fsib_row], preferred_element_type=F32)
        hn = tn // 2
        src = acc.at[pl.ds(pl.multiple_of(t0 + (1 - y) * hn, hn), hn)]
        rs[t] = go(remote(("rs", t), src, rbuf.at[pl.ds(t0 // 2, hn)], up))

    def combine(t):
        t0, tn = CHUNKS[t]
        hn = tn // 2
        rs[t].wait_recv()
        rows = pl.ds(pl.multiple_of(t0 + y * hn, hn), hn)
        total = acc[rows] + rbuf[pl.ds(t0 // 2, hn)]
        xn[row, rows] = (xg[row, rows].astype(F32) + total).astype(BF16)
        blk = xn.at[row, rows]
        for tag, dev in (("x", far), ("d", diag), ("y", up), ("s", sib)):
            xp[tag, t] = go(remote(("xn", tag, t), blk, blk, dev))

    outs = []

    def collect(t):
        t0, tn = CHUNKS[t]
        hn = tn // 2
        mine = pl.ds(pl.multiple_of(t0 + y * hn, hn), hn)
        other = pl.ds(pl.multiple_of(t0 + (1 - y) * hn, hn), hn)
        for tag, r, rows in (("y", row, other), ("x", far_row, mine), ("d", far_row, other)):
            xp[tag, t].wait_recv()
            blk = xn.at[r, rows]
            xf[tag, t] = go(remote(("xf2", tag, t), blk, blk, sib))
        c = local(("res", t), xn.at[row, pl.ds(t0, tn)], res_hbm.at[pl.ds(t0, tn)])
        c.start()
        outs.append(c)

    def finish(t):
        t0, tn = CHUNKS[t]
        xp["s", t].wait_recv()
        for tag in ("y", "x", "d"):
            xf[tag, t].wait_recv()
        norm(xn, g2, t0, tn)

    def project(t0, tn, i):
        rows = slice(t0, t0 + tn)
        out[rows] = jnp.dot(nb[rows], wq[...], preferred_element_type=F32).astype(BF16)
        c = local(("qkv", i), out.at[pl.ds(t0, tn)], qkv_hbm.at[pl.ds(t0, tn)])
        c.start()
        outs.append(c)

    down(0)
    down(1)
    combine(0)
    down(2)
    combine(1)
    collect(0)
    down(3)
    combine(2)
    collect(1)
    for c in loads["wq"]:
        c.wait()
    finish(0)
    finish(1)
    project(0, 128, 0)
    combine(3)
    collect(2)
    finish(2)
    collect(3)
    finish(3)
    project(128, 128, 1)
    for c in sent:
        c.wait_send()
    for c in outs:
        c.wait()


def solution(mesh):
    def per_device(residual, gain_mlp, gain_attn, w_gate, w_up, w_down, w_qkv):
        tokens, width = residual.shape
        ff = w_gate.shape[1]
        qkv = w_qkv.shape[1]
        hidden = width * 4
        any_spec = pl.BlockSpec(memory_space=pl.ANY)
        return pl.pallas_call(
            functools.partial(kernel, tokens, width, ff, Names(), Names()),
            out_shape=(jax.ShapeDtypeStruct((tokens, width), BF16), jax.ShapeDtypeStruct((tokens, qkv), BF16)),
            in_specs=[any_spec] * 7,
            out_specs=(any_spec, any_spec),
            scratch_shapes=[
                pltpu.VMEM((4, tokens, width), BF16),
                pltpu.VMEM((tokens, hidden), BF16),
                pltpu.VMEM((ff, hidden), BF16),
                pltpu.VMEM((ff, hidden), BF16),
                pltpu.VMEM((4, ff, width), BF16),
                pltpu.VMEM((hidden, qkv), BF16),
                pltpu.VMEM((4, tokens, ff), BF16),
                pltpu.VMEM((tokens, width), F32),
                pltpu.VMEM((tokens // 2, width), F32),
                pltpu.VMEM((4, tokens, width), BF16),
                pltpu.VMEM((4, 1, width), F32),
                pltpu.VMEM((4, 1, width), F32),
                pltpu.VMEM((tokens, qkv), BF16),
                pltpu.SemaphoreType.DMA((96,)),
                pltpu.SemaphoreType.DMA((96,)),
                pltpu.SemaphoreType.DMA((48,)),
            ],
            compiler_params=pltpu.CompilerParams(collective_id=0, has_side_effects=True, vmem_limit_bytes=67_000_000),
            name="block",
        )(residual, gain_mlp.reshape(1, width), gain_attn.reshape(1, width), w_gate.T, w_up.T, w_down, w_qkv)

    return jax.shard_map(
        per_device, mesh=mesh,
        in_specs=(P('data', 'row'), P('row'), P('row'), P(None, ('col', 'row')), P(None, ('col', 'row')),
                  P('col', 'row'), P(None, ('col', 'row'))),
        out_specs=(P('data', 'row'), P('data', ('col', 'row'))), check_vma=False)
```

```python
import functools

import jax
import jax.numpy as jnp
from jax import lax
from jax.experimental import pallas as pl
from jax.experimental.pallas import tpu as pltpu
from jax.sharding import PartitionSpec as P

NORM_EPS = 1e-6
MESH = pl.DeviceIdType.MESH
F32, BF16 = jnp.float32, jnp.bfloat16

SLICE = 128
RELAYED, DIRECT = 3, 5
NEAR = ((0, 352), (352, 336), (688, 352), (1040, 336))
WIDE = ((0, 688), (688, 688))
GROUPS = ((0, 384), (384, 384), (768, 384), (1152, 224))
BESIDE = ((("d", 0, 0),), (("d", 0, 1),), (("d", 1, 0),), (("d", 1, 1),), (("d", 2, 0), ("d", 2, 1), ("r", 0, 0), ("r", 0, 1)))
PASSES = (((("d", 0), ("d", 1)), ((), (("r", 1, 0),))),
          ((("d", 2), ("r", 0)), ((("d", 3, None),), (("r", 1, 1), ("r", 2, 0), ("d", 4, None)))),
          ((("d", 3), ("r", 1)), ((("r", 2, 1),), ())),
          ((("d", 4), ("r", 2)), ()))
CHUNK, CHUNKS = 32, 8
SPLIT_CHUNKS = (0,)
DIRECT_DIAG = (7,)
CUT = 4
STEPS = (
    "fwd0", "dfar0", "dfs0", "fwd1", "dfar1", "dfs1", "fwd2", "dfar2", "dfs2", "comb0", "fwd3", "dfar3",
    "dfs3", "comb1", "fwd4", "dfar4", "dfs4", "comb2", "fwd5", "dfar5", "cy0", "dfs5", "comb3", "fwd6",
    "dfar6", "cy1", "dfs6", "fwd7", "dfar7", "comb4", "cx0", "cy2", "dfs7", "cx1", "cx2", "comb5",
    "cd0", "cy3", "cx3", "fin0", "cd1", "comb6", "cx4", "cy4", "fin1", "cd2", "cx5", "comb7",
    "fin2", "cd3", "cy5", "cx6", "cy6", "fin3", "proj0", "cy7", "cd4", "cx7", "cd5", "cd7",
    "fin4", "cd6", "fin5", "fin7", "fin6", "proj1",
)
W_PARTS = 8


def dot(a, b):
    return jnp.dot(a, b, preferred_element_type=F32)


def dot_t(a, b):
    return lax.dot_general(a, b, (((1,), (1,)), ((), ())), preferred_element_type=F32)


def scoped(fn):
    @functools.wraps(fn)
    def run(*args):
        with jax.named_scope("#".join([fn.__name__] + [str(a) for a in args])):
            return fn(*args)
    return run


class Names:
    def __init__(self):
        self.table = {}

    def __call__(self, *key):
        return self.table.setdefault(key, len(self.table))


def kernel(tokens, width, ff, names, local_names,
           x_hbm, g1_hbm, g2_hbm, wg_hbm, wu_hbm, wd_hbm, wq_hbm, res, out,
           xg, nb, wg, wu, wd, wq, ag, acc, rbuf, xn, g1, g2, sq, scale, gacc, uacc, send_sem, recv_sem, loc_sem):
    data, y, row = lax.axis_index("data"), lax.axis_index("col"), lax.axis_index("row")
    cx = row // 2
    core = row - cx * 2
    sib_row = cx * 2 + 1 - core
    far_row = (1 - cx) * 2 + core
    fsib_row = (1 - cx) * 2 + 1 - core
    sib, far, fsib = (data, y, sib_row), (data, y, far_row), (data, y, fsib_row)
    up, diag = (data, 1 - y, row), (data, 1 - y, far_row)
    hidden = width * 4
    slices = width // SLICE

    def remote(key, src, dst, dev):
        i = names(*key)
        return pltpu.make_async_remote_copy(src_ref=src, dst_ref=dst, send_sem=send_sem.at[i], recv_sem=recv_sem.at[i],
                                            device_id=dev, device_id_type=MESH)

    def local(key, src, dst):
        return pltpu.make_async_copy(src, dst, loc_sem.at[local_names(*key)])

    sent = []

    def go(key, ref, dev):
        copy = remote(key, ref, ref, dev)
        copy.start()
        sent.append(copy)
        return copy

    own = [local(("x",), x_hbm, xg.at[row]), local(("g1",), g1_hbm, g1.at[row]), local(("g2",), g2_hbm, g2.at[row])]
    for c in own:
        c.start()
    loads = {}
    for name, src, dst in (("wg", wg_hbm, wg), ("wu", wu_hbm, wu)):
        loads[name] = [local((name, i), src.at[pl.ds(c0, cn)], dst.at[pl.ds(c0, cn)]) for i, (c0, cn) in enumerate(NEAR)]
    loads["wd"] = [local(("wd", i), wd_hbm.at[pl.ds(i * ff, ff)], wd.at[i]) for i in range(4)]
    part = hidden // W_PARTS
    loads["wq"] = [local(("wq", i), wq_hbm.at[pl.ds(i * part, part)], wq.at[pl.ds(i * part, part)]) for i in range(W_PARTS)]
    for pair in zip(loads["wg"], loads["wu"]):
        for c in pair:
            c.start()
    for name in ("wd", "wq"):
        for c in loads[name]:
            c.start()

    barrier = pltpu.get_barrier_semaphore()
    for dev in (sib, far, fsib, up, diag):
        pl.semaphore_signal(barrier, inc=1, device_id=dev, device_id_type=MESH)

    with jax.named_scope("own"):
        for c in own:
            c.wait()
        total = jnp.concatenate(
            [jnp.sum(jnp.square(xg[row, i:i + 64].astype(F32)), axis=1, keepdims=True) for i in range(0, tokens, 64)], axis=0)
        sq[row] = jnp.broadcast_to(total, (tokens, 128)).T[0:8]
    with jax.named_scope("barrier"):
        pl.semaphore_wait(barrier, 5)

    def cut(k):
        return pl.ds(pl.multiple_of(k * SLICE, SLICE), SLICE)

    def direct_slice(p):
        return y * (slices - RELAYED) + p if p < RELAYED else p

    def relayed_slice(q):
        return (1 - y) * (slices - RELAYED) + q

    def slice_of(item):
        return direct_slice(item[1]) if item[0] == "d" else relayed_slice(item[1])

    def parts(item):
        return (0, 1) if item[0] == "r" or item[1] < RELAYED else (None,)

    def x_block(b, item):
        toks = slice(None) if item[2] is None else pl.ds(item[2] * (tokens // 2), tokens // 2)
        return xg.at[b, toks, cut(slice_of(item))]

    gains = {}
    for name, ref in (("g1", g1), ("g2", g2)):
        for tag, dev in (("s", sib), ("f", far), ("fs", fsib)):
            gains[name, tag] = remote((name, tag), ref.at[row], ref.at[row], dev)
    small = [go(("sq", tag), sq.at[row], dev) for tag, dev in (("f", far), ("fs", fsib), ("s", sib))]
    x_sib = go(("xs",), xg.at[row], sib)
    x_in, x_fs = {}, {}
    for p in range(DIRECT):
        for h in parts(("d", p)):
            x_in["d", p, h] = go(("xx", p, h), x_block(row, ("d", p, h)), far)
        if p == 0:
            for c in gains.values():
                c.start()
                sent.append(c)

    def norm_slice(b, k):
        cols = pl.ds(pl.multiple_of(b * width + k * SLICE, SLICE), SLICE)
        nb[:, cols] = (xg[b, :, cut(k)].astype(F32) * scale[...] * g1[b, :, cut(k)]).astype(BF16)

    def norm_block(b):
        def step(k, carry):
            norm_slice(b, k)
            return carry
        lax.fori_loop(0, slices, step, 0)

    @scoped
    def relay(*item):
        x_in[item].wait_recv()
        blk = x_block(far_row, item)
        kind, p, h = item
        if kind == "d" and p < RELAYED:
            x_in["r", p, h] = go(("xy", p, h), blk, up)
        x_fs[item] = go(("xf",) + item, blk, sib)

    with jax.named_scope("stats"):
        for c in small:
            c.wait_recv()
        mean = (sq[0] + sq[1] + sq[2] + sq[3]) / hidden
        scale[...] = jnp.broadcast_to(lax.rsqrt(mean + NORM_EPS)[0:1], (128, tokens)).T
    with jax.named_scope("norm_own"):
        norm_block(row)
    with jax.named_scope("norm_sib"):
        gains["g1", "s"].wait_recv()
        x_sib.wait_recv()
        norm_block(sib_row)

    near = pl.ds(pl.multiple_of(cx * 2 * width, 2 * width), 2 * width)
    for item in BESIDE[0]:
        relay(*item)
    for g, (c0, cn) in enumerate(NEAR):
        cols = slice(c0, c0 + cn)
        with jax.named_scope(f"gu_near#{g}"):
            loads["wg"][g].wait()
            loads["wu"][g].wait()
            gacc[cols] = dot_t(wg[cols, near], nb[:, near])
            uacc[cols] = dot_t(wu[cols, near], nb[:, near])
        for item in BESIDE[1 + g]:
            relay(*item)
    for tag in ("f", "fs"):
        gains["g1", tag].wait_recv()

    a_sib, a_far, a_fs = {}, {}, {}

    def a_blocks(t):
        return [(g, c0, cn) for g, (c0, cn) in enumerate(GROUPS)] if t in SPLIT_CHUNKS else [(None, 0, ff)]

    def send_a(t, g, c0, cn):
        t0, tn = t * CHUNK, CHUNK
        a_far[t, g] = go(("ax", t, g), ag.at[row, pl.ds(t0, tn), pl.ds(c0, cn)], far)

    for i, (items, relays) in enumerate(PASSES):
        with jax.named_scope(f"norm_pass#{i}"):
            for item in items:
                norm_slice(far_row, slice_of(item))
            for item in items:
                for h in parts(item):
                    x_fs[item + (h,)].wait_recv()
                norm_slice(fsib_row, slice_of(item))
        where = [pl.ds(pl.multiple_of(b * width + slice_of(item) * SLICE, SLICE), SLICE)
                 for item in items for b in (far_row, fsib_row)]

        def product(w, cols):
            return dot_t(jnp.concatenate([w[cols, k] for k in where], axis=1), jnp.concatenate([nb[:, k] for k in where], axis=1))

        if i < len(PASSES) - 1:
            for g, (c0, cn) in enumerate(WIDE):
                cols = slice(c0, c0 + cn)
                with jax.named_scope(f"gu_pass#{i}#{g}"):
                    gate, upv = product(wg, cols), product(wu, cols)
                    gacc[cols] += gate
                    uacc[cols] += upv
                for item in relays[g]:
                    relay(*item)
            continue
        for g, (c0, cn) in enumerate(GROUPS):
            with jax.named_scope(f"gu_last#{g}"):
                cols = slice(c0, c0 + cn)
                gate = gacc[cols] + product(wg, cols)
                upv = uacc[cols] + product(wu, cols)
                ag[row, :, cols] = (jax.nn.silu(gate) * upv).astype(BF16).T
            for t in SPLIT_CHUNKS:
                send_a(t, g, c0, cn)
            a_sib[g] = go(("as", g), ag.at[row, :, pl.ds(c0, cn)], sib)
    for t in range(CHUNKS):
        if t not in SPLIT_CHUNKS:
            send_a(t, None, 0, ff)

    @scoped
    def forward(t):
        t0, tn = t * CHUNK, CHUNK
        for g, c0, cn in a_blocks(t):
            a_far[t, g].wait_recv()
            a_fs[t, g] = go(("af", t, g), ag.at[far_row, pl.ds(t0, tn), pl.ds(c0, cn)], sib)

    for c in loads["wd"]:
        c.wait()
    with jax.named_scope("down_own"):
        acc[...] = dot(ag[row], wd[row])
    with jax.named_scope("down_sib"):
        for c in a_sib.values():
            c.wait_recv()
        acc[...] += dot(ag[sib_row], wd[sib_row])

    rs, xp, xf = {}, {}, {}

    def halves(t):
        t0, tn = t * CHUNK, CHUNK
        hn = tn // 2
        return (pl.ds(pl.multiple_of(t0 + y * hn, hn), hn), pl.ds(pl.multiple_of(t0 + (1 - y) * hn, hn), hn),
                pl.ds(t0 // 2, hn))

    @scoped
    def down_far(t):
        rows = slice(t * CHUNK, (t + 1) * CHUNK)
        acc[rows] += dot(ag[far_row, rows], wd[far_row])

    @scoped
    def down_fsib(t):
        rows = slice(t * CHUNK, (t + 1) * CHUNK)
        for g, _, _ in a_blocks(t):
            a_fs[t, g].wait_recv()
        acc[rows] += dot(ag[fsib_row, rows], wd[fsib_row])
        _, other, packed = halves(t)
        rs[t] = remote(("rs", t), acc.at[other], rbuf.at[packed], up)
        rs[t].start()
        sent.append(rs[t])

    @scoped
    def combine(t):
        mine, _, packed = halves(t)
        rs[t].wait_recv()
        xn[row, mine] = (xg[row, mine].astype(F32) + (acc[mine] + rbuf[packed])).astype(BF16)
        blk = xn.at[row, mine]
        targets = [("y", up), ("x", far), ("s", sib)] + ([("d", diag)] if t in DIRECT_DIAG else [])
        for tag, dev in targets:
            xp[tag, t] = go(("xn", tag, t), blk, dev)

    @scoped
    def collect(tag, t):
        mine, other, _ = halves(t)
        r, rows = {"y": (row, other), "x": (far_row, mine), "d": (far_row, other)}[tag]
        xp[tag, t].wait_recv()
        blk = xn.at[r, rows]
        if tag == "y" and t not in DIRECT_DIAG:
            xp["d", t] = go(("xn", "d", t), blk, far)
        xf[tag, t] = go(("xf2", tag, t), blk, sib)

    @scoped
    def finish(t):
        t0, tn = t * CHUNK, CHUNK
        xp["s", t].wait_recv()
        for tag in ("y", "x", "d"):
            xf[tag, t].wait_recv()
        res[pl.ds(t0, tn)] = xn[row, pl.ds(t0, tn)]

        def step(i, carry):
            rows = pl.ds(pl.multiple_of(t0 + i * 16, 16), 16)
            blocks = [xn[b, rows].astype(F32) for b in range(4)]
            total = sum(jnp.sum(v * v, axis=1, keepdims=True) for v in blocks)
            r = lax.rsqrt(total / hidden + NORM_EPS)
            for b in range(4):
                nb[rows, b * width:(b + 1) * width] = (blocks[b] * r * g2[b]).astype(BF16)
            return carry
        lax.fori_loop(0, tn // 16, step, 0)

    @scoped
    def project(i):
        if i == 0:
            for c in loads["wq"]:
                c.wait()
        rows = slice(0, CUT * CHUNK) if i == 0 else slice(CUT * CHUNK, tokens)
        out[rows] = dot(nb[rows], wq[...]).astype(BF16)

    for tag in ("s", "f", "fs"):
        gains["g2", tag].wait_recv()
    steps = {"fwd": forward, "dfar": down_far, "dfs": down_fsib, "comb": combine, "cy": functools.partial(collect, "y"),
             "cx": functools.partial(collect, "x"), "cd": functools.partial(collect, "d"), "fin": finish, "proj": project}
    for name in STEPS:
        steps[name[:-1]](int(name[-1]))
    with jax.named_scope("drain"):
        for c in sent:
            c.wait_send()


def solution(mesh):
    def per_device(residual, gain_mlp, gain_attn, w_gate, w_up, w_down, w_qkv):
        tokens, width = residual.shape
        ff = w_gate.shape[1]
        qkv = w_qkv.shape[1]
        hidden = width * 4
        any_spec = pl.BlockSpec(memory_space=pl.ANY)
        return pl.pallas_call(
            functools.partial(kernel, tokens, width, ff, Names(), Names()),
            out_shape=(pltpu.VMEM((tokens, width), BF16), pltpu.VMEM((tokens, qkv), BF16)),
            in_specs=[any_spec] * 7,
            out_specs=(pl.BlockSpec(memory_space=pltpu.VMEM),) * 2,
            scratch_shapes=[
                pltpu.VMEM((4, tokens, width), BF16),
                pltpu.VMEM((tokens, hidden), BF16),
                pltpu.VMEM((ff, hidden), BF16),
                pltpu.VMEM((ff, hidden), BF16),
                pltpu.VMEM((4, ff, width), BF16),
                pltpu.VMEM((hidden, qkv), BF16),
                pltpu.VMEM((4, tokens, ff), BF16),
                pltpu.VMEM((tokens, width), F32),
                pltpu.VMEM((tokens // 2, width), F32),
                pltpu.VMEM((4, tokens, width), BF16),
                pltpu.VMEM((4, 1, width), F32),
                pltpu.VMEM((4, 1, width), F32),
                pltpu.VMEM((4, 8, tokens), F32),
                pltpu.VMEM((tokens, 128), F32),
                pltpu.VMEM((ff, tokens), F32),
                pltpu.VMEM((ff, tokens), F32),
                pltpu.SemaphoreType.DMA((160,)),
                pltpu.SemaphoreType.DMA((160,)),
                pltpu.SemaphoreType.DMA((32,)),
            ],
            compiler_params=pltpu.CompilerParams(collective_id=0, has_side_effects=True, vmem_limit_bytes=65_500_000),
            name="block",
        )(residual, gain_mlp.reshape(1, width), gain_attn.reshape(1, width), w_gate.T, w_up.T, w_down, w_qkv)

    return jax.shard_map(
        per_device, mesh=mesh,
        in_specs=(P('data', 'row'), P('row'), P('row'), P(None, ('col', 'row')), P(None, ('col', 'row')),
                  P('col', 'row'), P(None, ('col', 'row'))),
        out_specs=(P('data', 'row'), P('data', ('col', 'row'))), check_vma=False)
```

```python
import functools
import math

import jax
import jax.numpy as jnp
from jax import lax
from jax.experimental import pallas as pl
from jax.experimental.pallas import tpu as pltpu
from jax.sharding import PartitionSpec as P

NORM_EPS = 1e-6
MESH = pl.DeviceIdType.MESH
F32, BF16 = jnp.float32, jnp.bfloat16

SLICE = 128
RELAYED, DIRECT = 3, 5
NEAR = ((0, 352), (352, 336), (688, 352), (1040, 336))
WIDE = ((0, 688), (688, 688))
GROUPS = ((0, 384), (384, 384), (768, 384), (1152, 224))
BESIDE = ((("d", 0, 0),), (("d", 0, 1),), (("d", 1, 0),), (("d", 1, 1), ("d", 2, 0)), (("d", 2, 1), ("r", 0, 0)))
PASSES = (((("d", 0), ("d", 1)), ((("r", 0, 1),), (("r", 1, 0), ("d", 3, None)))),
          ((("d", 2), ("r", 0)), ((("r", 1, 1),), (("d", 4, None), ("r", 2, 0)))),
          ((("d", 3), ("r", 1)), ((("r", 2, 1),), ())),
          ((("d", 4), ("r", 2)), ()))
CHUNK, CHUNKS = 32, 8
SPLIT_CHUNKS = (0,)
DIAGONAL = "xxxxxydd"
CUT = 4
STEPS = (
    "fwd0", "dfar0", "dfs0", "fwd1", "dfar1", "dfs1", "fwd2", "dfar2", "dfs2", "comb0", "fwd3", "dfar3",
    "dfs3", "comb1", "fwd4", "dfar4", "dfs4", "comb2", "fwd5", "dfar5", "cy0", "dfs5", "comb3", "fwd6",
    "dfar6", "cy1", "dfs6", "fwd7", "dfar7", "comb4", "cx0", "cy2", "dfs7", "cx1", "cx2", "comb5",
    "cd0", "cy3", "cx3", "fin0", "cd1", "comb6", "cx4", "cy4", "fin1", "cd2", "cx5", "comb7",
    "fin2", "cd3", "cy5", "cx6", "cy6", "fin3", "proj0", "cy7", "cd4", "cd5", "cd6", "cx7",
    "fin4", "cd7", "fin5", "fin6", "fin7",
)
W_PARTS = 8


def dot(a, b):
    return jnp.dot(a, b, preferred_element_type=F32)


def dot_t(a, b):
    return lax.dot_general(a, b, (((1,), (1,)), ((), ())), preferred_element_type=F32)


def scoped(fn):
    @functools.wraps(fn)
    def run(*args):
        with jax.named_scope("#".join([fn.__name__] + [str(a) for a in args])):
            return fn(*args)
    return run


class Names:
    def __init__(self):
        self.table = {}

    def __call__(self, *key):
        return self.table.setdefault(key, len(self.table))


def kernel(tokens, width, ff, names, local_names,
           x_hbm, g1_hbm, g2_hbm, wg_hbm, wu_hbm, wd_hbm, wq_hbm, res, out, nb, wq,
           xg, wg, wu, wd, ag, acc, rbuf, xn, gains, sq, scale, gacc, uacc, send_sem, recv_sem, loc_sem):
    data, y, row = lax.axis_index("data"), lax.axis_index("col"), lax.axis_index("row")
    cx = row // 2
    core = row - cx * 2
    sib_row = cx * 2 + 1 - core
    far_row = (1 - cx) * 2 + core
    fsib_row = (1 - cx) * 2 + 1 - core
    sib, far, fsib = (data, y, sib_row), (data, y, far_row), (data, y, fsib_row)
    up, diag = (data, 1 - y, row), (data, 1 - y, far_row)
    hidden = width * 4
    wide = ag.shape[2]
    slices = width // SLICE

    def remote(key, src, dst, dev):
        return pltpu.make_async_remote_copy(src_ref=src, dst_ref=dst, send_sem=send_sem.at[1 if key[0] == "sq" else 0], recv_sem=recv_sem.at[names(*key)],
                                            device_id=dev, device_id_type=MESH)

    def local(key, src, dst):
        return pltpu.make_async_copy(src, dst, loc_sem.at[local_names(*key)])

    def arrived(key, like):
        pltpu.make_async_copy(like, like, recv_sem.at[names(*key)]).wait()

    def loaded(key, like):
        pltpu.make_async_copy(like, like, loc_sem.at[local_names(*key)]).wait()

    sent = []

    def go(key, ref, dev, dst=None):
        copy = remote(key, ref, ref if dst is None else dst, dev)
        copy.start()
        if key[0] != "sq":
            sent.append(math.prod(ref.shape) * jnp.dtype(ref.dtype).itemsize)
        return copy

    own = [local(("x",), x_hbm, xg.at[row]), local(("g1",), g1_hbm, gains.at[row, 0]), local(("g2",), g2_hbm, gains.at[row, 1])]
    for c in own:
        c.start()
    for g, (c0, cn) in enumerate(NEAR):
        for src, dst in ((wg_hbm, wg), (wu_hbm, wu)):
            local(("w", g), src.at[pl.ds(c0, cn)], dst.at[pl.ds(c0, cn)]).start()
    for i in range(4):
        local(("wd",), wd_hbm.at[pl.ds(i * ff, ff)], wd.at[i]).start()
    part = hidden // W_PARTS
    for i in range(W_PARTS):
        local(("wq",), wq_hbm.at[pl.ds(i * part, part)], wq.at[pl.ds(i * part, part)]).start()

    barrier = pltpu.get_barrier_semaphore()
    for dev in (sib, far, fsib, up, diag):
        pl.semaphore_signal(barrier, inc=1, device_id=dev, device_id_type=MESH)

    with jax.named_scope("own"):
        if wide > ff:
            ag[row, :, ff:] = jnp.zeros((tokens, wide - ff), BF16)
        for c in own:
            c.wait()
        part = sum(jnp.square(xg[row, :, i:i + 128].astype(F32)) for i in range(0, width, 128)).T
        sq[row] = jnp.sum(part, axis=0, keepdims=True)
    with jax.named_scope("barrier"):
        pl.semaphore_wait(barrier, 5)

    def cut(k):
        return pl.ds(pl.multiple_of(k * SLICE, SLICE), SLICE)

    def direct_slice(p):
        return y * (slices - RELAYED) + p if p < RELAYED else p

    def relayed_slice(q):
        return (1 - y) * (slices - RELAYED) + q

    def slice_of(item):
        return direct_slice(item[1]) if item[0] == "d" else relayed_slice(item[1])

    def parts(item):
        return (0, 1) if item[0] == "r" or item[1] < RELAYED else (None,)

    def x_block(b, item):
        toks = slice(None) if item[2] is None else pl.ds(item[2] * (tokens // 2), tokens // 2)
        return xg.at[b, toks, cut(slice_of(item))]

    x_in = {}
    pass_of = {item: i for i, (items, _) in enumerate(PASSES) for item in items}

    def send_x(p):
        for h in parts(("d", p)):
            x_in["d", p, h] = go(("xx", p, h), x_block(row, ("d", p, h)), far)

    for dev in (far, fsib, sib):
        go(("sq",), sq.at[row], dev)
    x_sib = go(("xs",), xg.at[row], sib)
    go(("gs",), gains.at[row], sib)
    send_x(0)
    for dev in (far, fsib):
        go(("g1",), gains.at[row, 0], dev)
    for p in range(1, DIRECT):
        send_x(p)
    for dev in (far, fsib):
        go(("g2",), gains.at[row, 1], dev)

    def norm_slice(b, k):
        cols = pl.ds(pl.multiple_of(b * width + k * SLICE, SLICE), SLICE)
        nb[:, cols] = (xg[b, :, cut(k)].astype(F32) * scale[...] * gains[b, 0, :, cut(k)]).astype(BF16)

    def norm_block(b):
        def step(k, carry):
            norm_slice(b, k)
            return carry
        lax.fori_loop(0, slices, step, 0)

    @scoped
    def relay(*item):
        x_in[item].wait_recv()
        blk = x_block(far_row, item)
        kind, p, h = item
        if kind == "d" and p < RELAYED:
            x_in["r", p, h] = go(("xy", p, h), blk, up)
        go(("xf", pass_of[kind, p]), blk, sib)

    with jax.named_scope("stats"):
        arrived(("sq",), sq.at[pl.ds(0, 3)])
        mean = (sq[0] + sq[1] + sq[2] + sq[3]) / hidden
        scale[...] = jnp.broadcast_to(lax.rsqrt(mean + NORM_EPS), (128, tokens)).T
    with jax.named_scope("norm_own"):
        norm_block(row)
    with jax.named_scope("norm_sib"):
        x_sib.wait_recv()
        arrived(("gs",), gains.at[0])
        norm_block(sib_row)

    near = pl.ds(pl.multiple_of(cx * 2 * width, 2 * width), 2 * width)
    for item in BESIDE[0]:
        relay(*item)
    for g, (c0, cn) in enumerate(NEAR):
        cols = slice(c0, c0 + cn)
        with jax.named_scope(f"gu_near#{g}"):
            loaded(("w", g), wg.at[pl.ds(0, 2 * cn)])
            gacc[cols] = dot_t(wg[cols, near], nb[:, near])
            uacc[cols] = dot_t(wu[cols, near], nb[:, near])
        for item in BESIDE[1 + g]:
            relay(*item)
    arrived(("g1",), gains.at[0])

    def send_a(t, c0, cn):
        go(("ax", t), ag.at[row, pl.ds(t * CHUNK, CHUNK), pl.ds(c0, cn)], far)

    for i, (items, relays) in enumerate(PASSES):
        with jax.named_scope(f"norm_pass#{i}"):
            for item in items:
                norm_slice(far_row, slice_of(item))
            arrived(("xf", i), xg.at[0, :, pl.ds(0, len(items) * SLICE)])
            for item in items:
                norm_slice(fsib_row, slice_of(item))
        where = [pl.ds(pl.multiple_of(b * width + slice_of(item) * SLICE, SLICE), SLICE)
                 for item in items for b in (far_row, fsib_row)]

        def product(w, cols):
            return dot_t(jnp.concatenate([w[cols, k] for k in where], axis=1), jnp.concatenate([nb[:, k] for k in where], axis=1))

        if i < len(PASSES) - 1:
            for g, (c0, cn) in enumerate(WIDE):
                cols = slice(c0, c0 + cn)
                with jax.named_scope(f"gu_pass#{i}#{g}"):
                    gate, upv = product(wg, cols), product(wu, cols)
                    gacc[cols] += gate
                    uacc[cols] += upv
                for item in relays[g]:
                    relay(*item)
            continue
        for g, (c0, cn) in enumerate(GROUPS):
            with jax.named_scope(f"gu_last#{g}"):
                cols = slice(c0, c0 + cn)
                gate = gacc[cols] + product(wg, cols)
                upv = uacc[cols] + product(wu, cols)
                ag[row, :, cols] = (jax.nn.silu(gate) * upv).astype(BF16).T
            sent_cn = cn if c0 + cn < ff else wide - c0
            for t in SPLIT_CHUNKS:
                send_a(t, c0, sent_cn)
            go(("as",), ag.at[row, :, pl.ds(c0, sent_cn)], sib)
    for t in range(CHUNKS):
        if t not in SPLIT_CHUNKS:
            send_a(t, 0, wide)

    @scoped
    def forward(t):
        blk = ag.at[far_row, pl.ds(t * CHUNK, CHUNK)]
        arrived(("ax", t), blk)
        go(("af", t), blk, sib)

    loaded(("wd",), wd)
    with jax.named_scope("down_own"):
        acc[...] = dot(ag[row, :, :ff], wd[row])
    with jax.named_scope("down_sib"):
        arrived(("as",), ag.at[sib_row])
        acc[...] += dot(ag[sib_row, :, :ff], wd[sib_row])

    rs, xp = {}, {}

    def halves(t):
        t0, tn = t * CHUNK, CHUNK
        hn = tn // 2
        return (pl.ds(pl.multiple_of(t0 + y * hn, hn), hn), pl.ds(pl.multiple_of(t0 + (1 - y) * hn, hn), hn),
                pl.ds(t0 // 2, hn))

    @scoped
    def down_far(t):
        rows = slice(t * CHUNK, (t + 1) * CHUNK)
        acc[rows] += dot(ag[far_row, rows, :ff], wd[far_row])

    @scoped
    def down_fsib(t):
        rows = slice(t * CHUNK, (t + 1) * CHUNK)
        arrived(("af", t), ag.at[fsib_row, pl.ds(t * CHUNK, CHUNK)])
        acc[rows] += dot(ag[fsib_row, rows, :ff], wd[fsib_row])
        _, other, packed = halves(t)
        rs[t] = go(("rs", t), acc.at[other], up, rbuf.at[packed])

    @scoped
    def combine(t):
        mine, _, packed = halves(t)
        rs[t].wait_recv()
        xn[row, mine] = (xg[row, mine].astype(F32) + (acc[mine] + rbuf[packed])).astype(BF16)
        blk = xn.at[row, mine]
        targets = [("y", up), ("x", far), ("s", sib)] + ([("d", diag)] if DIAGONAL[t] == "d" else [])
        for tag, dev in targets:
            xp[tag, t] = go(("xn", "s", t) if tag == "s" else ("xn", tag, t), blk, dev)

    @scoped
    def collect(tag, t):
        mine, other, _ = halves(t)
        r, rows = {"y": (row, other), "x": (far_row, mine), "d": (far_row, other)}[tag]
        xp[tag, t].wait_recv()
        blk = xn.at[r, rows]
        if (tag, DIAGONAL[t]) in (("y", "x"), ("x", "y")):
            xp["d", t] = go(("xn", "d", t), blk, far if tag == "y" else up)
        go(("xn", "s", t), blk, sib)

    @scoped
    def finish(t):
        t0, tn = t * CHUNK, CHUNK
        arrived(("xn", "s", t), xn.at[0, pl.ds(0, 2 * CHUNK)])
        res[pl.ds(t0, tn)] = xn[row, pl.ds(t0, tn)]

        def step(i, carry):
            rows = pl.ds(pl.multiple_of(t0 + i * 16, 16), 16)
            blocks = [xn[b, rows].astype(F32) for b in range(4)]
            total = sum(jnp.sum(v * v, axis=1, keepdims=True) for v in blocks)
            r = lax.rsqrt(total / hidden + NORM_EPS)
            for b in range(4):
                nb[rows, b * width:(b + 1) * width] = (blocks[b] * r * gains[b, 1]).astype(BF16)
            return carry
        lax.fori_loop(0, tn // 16, step, 0)

    @scoped
    def project(i):
        loaded(("wq",), wq)
        out[...] = dot(nb[:CUT * CHUNK], wq[...]).astype(BF16)

    arrived(("g2",), gains.at[0])
    steps = {"fwd": forward, "dfar": down_far, "dfs": down_fsib, "comb": combine, "cy": functools.partial(collect, "y"),
             "cx": functools.partial(collect, "x"), "cd": functools.partial(collect, "d"), "fin": finish, "proj": project}
    for name in STEPS:
        steps[name[:-1]](int(name[-1]))
    with jax.named_scope("drain"):
        pltpu.make_async_copy(sq.at[pl.ds(0, 3)], sq.at[pl.ds(0, 3)], send_sem.at[1]).wait()
        tiles = sum(sent) // (16 * 128 * 2)
        deep = max(d for d in range(1, ff // 16 + 1) if tiles % d == 0)
        like = wg.at[pl.ds(0, deep * 16), pl.ds(0, tiles // deep * 128)]
        pltpu.make_async_copy(like, like, send_sem.at[0]).wait()


def last_kernel(res, first, nb, wq, res_hbm, qkv_hbm, out, sem):
    t0, part = CUT * CHUNK, wq.shape[1] // 2
    copies = [pltpu.make_async_copy(res, res_hbm, sem.at[0]),
              pltpu.make_async_copy(first, qkv_hbm.at[pl.ds(0, t0)], sem.at[1])]
    for c in copies:
        c.start()
    for i in range(2):
        cols = pl.ds(i * part, part)
        out[:, cols] = dot(nb[t0:], wq[:, cols]).astype(BF16)
        c = pltpu.make_async_copy(out.at[:, cols], qkv_hbm.at[pl.ds(t0, out.shape[0]), cols], sem.at[2 + i])
        c.start()
        copies.append(c)
    for c in copies:
        c.wait()


def solution(mesh):
    def per_device(residual, gain_mlp, gain_attn, w_gate, w_up, w_down, w_qkv):
        tokens, width = residual.shape
        ff = w_gate.shape[1]
        qkv = w_qkv.shape[1]
        hidden = width * 4
        any_spec = pl.BlockSpec(memory_space=pl.ANY)
        vmem_spec = pl.BlockSpec(memory_space=pltpu.VMEM)
        held = pl.pallas_call(
            functools.partial(kernel, tokens, width, ff, Names(), Names()),
            out_shape=(pltpu.VMEM((tokens, width), BF16), pltpu.VMEM((CUT * CHUNK, qkv), BF16),
                       pltpu.VMEM((tokens, hidden), BF16), pltpu.VMEM((hidden, qkv), BF16)),
            in_specs=[any_spec] * 7,
            out_specs=(vmem_spec,) * 4,
            scratch_shapes=[
                pltpu.VMEM((4, tokens, width), BF16),
                pltpu.VMEM((ff, hidden), BF16),
                pltpu.VMEM((ff, hidden), BF16),
                pltpu.VMEM((4, ff, width), BF16),
                pltpu.VMEM((4, tokens, (ff + 127) // 128 * 128), BF16),
                pltpu.VMEM((tokens, width), F32),
                pltpu.VMEM((tokens // 2, width), F32),
                pltpu.VMEM((4, tokens, width), BF16),
                pltpu.VMEM((4, 2, 1, width), F32),
                pltpu.VMEM((4, 1, tokens), F32),
                pltpu.VMEM((tokens, 128), F32),
                pltpu.VMEM((ff, tokens), F32),
                pltpu.VMEM((ff, tokens), F32),
                pltpu.SemaphoreType.DMA((2,)),
                pltpu.SemaphoreType.DMA((81,)),
                pltpu.SemaphoreType.DMA((11,)),
            ],
            compiler_params=pltpu.CompilerParams(collective_id=0, has_side_effects=True, vmem_limit_bytes=50_000_000),
            name="block",
        )(residual, gain_mlp.reshape(1, width), gain_attn.reshape(1, width), w_gate.T, w_up.T, w_down, w_qkv)
        return pl.pallas_call(
            last_kernel,
            out_shape=(jax.ShapeDtypeStruct((tokens, width), BF16), jax.ShapeDtypeStruct((tokens, qkv), BF16)),
            in_specs=[vmem_spec] * 4,
            out_specs=(any_spec,) * 2,
            scratch_shapes=[pltpu.VMEM((tokens - CUT * CHUNK, qkv), BF16), pltpu.SemaphoreType.DMA((4,))],
            compiler_params=pltpu.CompilerParams(vmem_limit_bytes=16_000_000),
            name="last",
        )(*(pltpu.with_memory_space_constraint(v, pltpu.VMEM) for v in held))

    return jax.shard_map(
        per_device, mesh=mesh,
        in_specs=(P('data', 'row'), P('row'), P('row'), P(None, ('col', 'row')), P(None, ('col', 'row')),
                  P('col', 'row'), P(None, ('col', 'row'))),
        out_specs=(P('data', 'row'), P('data', ('col', 'row'))), check_vma=False)
```

```python
import functools
import math

import jax
import jax.numpy as jnp
from jax import lax
from jax.experimental import pallas as pl
from jax.experimental.pallas import tpu as pltpu
from jax.sharding import PartitionSpec as P

NORM_EPS = 1e-6
MESH = pl.DeviceIdType.MESH
F32, BF16 = jnp.float32, jnp.bfloat16

SLICE = 128
RELAYED, DIRECT = 3, 5
NEAR = ((0, 352), (352, 336), (688, 352), (1040, 336))
WIDE = ((0, 688), (688, 688))
GROUPS = ((0, 384), (384, 384), (768, 384), (1152, 224))
BESIDE = ((("d", 0, 0),), (("d", 0, 1),), (("d", 1, 0),), (("d", 1, 1), ("d", 2, 0)), (("d", 2, 1), ("r", 0, 0)))
PASSES = (((("d", 0), ("d", 1)), ((("r", 0, 1),), (("r", 1, 0), ("d", 3, None)))),
          ((("d", 2), ("r", 0)), ((("r", 1, 1),), (("d", 4, None), ("r", 2, 0)))),
          ((("d", 3), ("r", 1)), ((("r", 2, 1),), ())),
          ((("d", 4), ("r", 2)), ()))
CHUNK, CHUNKS = 32, 8
SPLIT_CHUNKS = (0,)
DIAGONAL = "xxxxyxyd"
LATE_PARTS = 1
CUT = 4
STEPS = (
    "fwd0", "dfar0", "dfs0", "fwd1", "dfar1", "dfs1", "fwd2", "dfar2", "dfs2", "comb0", "sy0", "fwd3",
    "dfar3", "dfs3", "comb1", "sy1", "fwd4", "dfar4", "dfs4", "comb2", "sy2", "fwd5", "dfar5", "cy0",
    "dfs5", "comb3", "sy3", "fwd6", "dfar6", "cy1", "dfs6", "fwd7", "comb4", "sy4", "dfar7", "cx0",
    "cy2", "dfs7", "cx1", "cx2", "comb5", "sy5", "cd0", "cy3", "cx3", "fin0", "cd1", "comb6",
    "sy6", "cx4", "cy4", "fin1", "cd2", "cx5", "comb7", "sy7", "fin2", "cd3", "cy5", "cx6",
    "cy6", "fin3", "cd4", "proj0", "proj1", "cy7", "cx7", "fin4", "cd5", "cd6", "cd7", "proj2",
    "fin5", "fin6", "fin7",
)
W_PARTS = 8


def dot(a, b):
    return jnp.dot(a, b, preferred_element_type=F32)


def dot_t(a, b):
    return lax.dot_general(a, b, (((1,), (1,)), ((), ())), preferred_element_type=F32)


def scoped(fn):
    @functools.wraps(fn)
    def run(*args):
        with jax.named_scope("#".join([fn.__name__] + [str(a) for a in args])):
            return fn(*args)
    return run


class Names:
    def __init__(self):
        self.table = {}

    def __call__(self, *key):
        return self.table.setdefault(earlier(key), len(self.table))


def earlier(key):
    if key[0] != "xn":
        return key
    tag, t = key[1:]
    if tag == "x":
        return ("xx",) + ((t // 2, t % 2) if t < 2 * RELAYED else (t - RELAYED, None))
    if tag == "y":
        return ("xy", t // 2, t % 2) if t < 2 * RELAYED else ("rs", t - 2 * RELAYED, 0)
    if tag == "s":
        return ("as",) if t == 0 else ("af", t - 1)
    return ("xf", t) if t < len(PASSES) else (("sq",), ("xs",), ("gs",), ("g1",))[t - len(PASSES)]


def kernel(tokens, width, ff, names, local_names,
           x_hbm, g1_hbm, g2_hbm, wg_hbm, wu_hbm, wd_hbm, wq_hbm, res, out, nb, wq,
           xg, wg, wu, wd, ag, acc, rbuf, xn, gains, sq, scale, gacc, uacc, send_sem, recv_sem, loc_sem):
    data, y, row = lax.axis_index("data"), lax.axis_index("col"), lax.axis_index("row")
    cx = row // 2
    core = row - cx * 2
    sib_row = cx * 2 + 1 - core
    far_row = (1 - cx) * 2 + core
    fsib_row = (1 - cx) * 2 + 1 - core
    sib, far, fsib = (data, y, sib_row), (data, y, far_row), (data, y, fsib_row)
    up, diag = (data, 1 - y, row), (data, 1 - y, far_row)
    hidden = width * 4
    wide = ag.shape[2]
    slices = width // SLICE

    def remote(key, src, dst, dev):
        return pltpu.make_async_remote_copy(src_ref=src, dst_ref=dst, send_sem=send_sem.at[1 if key[0] == "sq" else 0], recv_sem=recv_sem.at[names(*key)],
                                            device_id=dev, device_id_type=MESH)

    def local(key, src, dst):
        return pltpu.make_async_copy(src, dst, loc_sem.at[local_names(*key)])

    def arrived(key, like):
        pltpu.make_async_copy(like, like, recv_sem.at[names(*key)]).wait()

    def loaded(key, like):
        pltpu.make_async_copy(like, like, loc_sem.at[local_names(*key)]).wait()

    sent = []

    def go(key, ref, dev, dst=None):
        copy = remote(key, ref, ref if dst is None else dst, dev)
        copy.start()
        if key[0] != "sq":
            sent.append(math.prod(ref.shape) * jnp.dtype(ref.dtype).itemsize)
        return copy

    own = [local(("x",), x_hbm, xg.at[row]), local(("g1",), g1_hbm, gains.at[row, 0]), local(("g2",), g2_hbm, gains.at[row, 1])]
    for c in own:
        c.start()
    for g, (c0, cn) in enumerate(NEAR):
        for src, dst in ((wg_hbm, wg), (wu_hbm, wu)):
            local(("w", g), src.at[pl.ds(c0, cn)], dst.at[pl.ds(c0, cn)]).start()
    for i in range(4):
        local(("wd",), wd_hbm.at[pl.ds(i * ff, ff)], wd.at[i]).start()
    part = hidden // W_PARTS
    for i in range(W_PARTS):
        local(("wq",), wq_hbm.at[pl.ds(i * part, part)], wq.at[pl.ds(i * part, part)]).start()

    barrier = pltpu.get_barrier_semaphore()
    for dev in (sib, far, fsib, up, diag):
        pl.semaphore_signal(barrier, inc=1, device_id=dev, device_id_type=MESH)

    with jax.named_scope("own"):
        if wide > ff:
            ag[row, :, ff:] = jnp.zeros((tokens, wide - ff), BF16)
        for c in own:
            c.wait()
        part = sum(jnp.square(xg[row, :, i:i + 128].astype(F32)) for i in range(0, width, 128)).T
        sq[row] = jnp.sum(part, axis=0, keepdims=True)
    with jax.named_scope("barrier"):
        pl.semaphore_wait(barrier, 5)

    def cut(k):
        return pl.ds(pl.multiple_of(k * SLICE, SLICE), SLICE)

    def direct_slice(p):
        return y * (slices - RELAYED) + p if p < RELAYED else p

    def relayed_slice(q):
        return (1 - y) * (slices - RELAYED) + q

    def slice_of(item):
        return direct_slice(item[1]) if item[0] == "d" else relayed_slice(item[1])

    def parts(item):
        return (0, 1) if item[0] == "r" or item[1] < RELAYED else (None,)

    def x_block(b, item):
        toks = slice(None) if item[2] is None else pl.ds(item[2] * (tokens // 2), tokens // 2)
        return xg.at[b, toks, cut(slice_of(item))]

    x_in = {}
    pass_of = {item: i for i, (items, _) in enumerate(PASSES) for item in items}

    def send_x(p):
        for h in parts(("d", p)):
            x_in["d", p, h] = go(("xx", p, h), x_block(row, ("d", p, h)), far)

    for dev in (far, fsib, sib):
        go(("sq",), sq.at[row], dev)
    x_sib = go(("xs",), xg.at[row], sib)
    go(("gs",), gains.at[row], sib)
    send_x(0)
    for dev in (far, fsib):
        go(("g1",), gains.at[row, 0], dev)
    for p in range(1, DIRECT):
        send_x(p)
    for dev in (far, fsib):
        go(("g2",), gains.at[row, 1], dev)

    def norm_slice(b, k):
        cols = pl.ds(pl.multiple_of(b * width + k * SLICE, SLICE), SLICE)
        nb[:, cols] = (xg[b, :, cut(k)].astype(F32) * scale[...] * gains[b, 0, :, cut(k)]).astype(BF16)

    def norm_block(b):
        def step(k, carry):
            norm_slice(b, k)
            return carry
        lax.fori_loop(0, slices, step, 0)

    @scoped
    def relay(*item):
        x_in[item].wait_recv()
        blk = x_block(far_row, item)
        kind, p, h = item
        if kind == "d" and p < RELAYED:
            x_in["r", p, h] = go(("xy", p, h), blk, up)
        go(("xf", pass_of[kind, p]), blk, sib)

    with jax.named_scope("stats"):
        arrived(("sq",), sq.at[pl.ds(0, 3)])
        mean = (sq[0] + sq[1] + sq[2] + sq[3]) / hidden
        scale[...] = jnp.broadcast_to(lax.rsqrt(mean + NORM_EPS), (128, tokens)).T
    with jax.named_scope("norm_own"):
        norm_block(row)
    with jax.named_scope("norm_sib"):
        x_sib.wait_recv()
        arrived(("gs",), gains.at[0])
        norm_block(sib_row)

    near = pl.ds(pl.multiple_of(cx * 2 * width, 2 * width), 2 * width)
    for item in BESIDE[0]:
        relay(*item)
    for g, (c0, cn) in enumerate(NEAR):
        cols = slice(c0, c0 + cn)
        with jax.named_scope(f"gu_near#{g}"):
            loaded(("w", g), wg.at[pl.ds(0, 2 * cn)])
            gacc[cols] = dot_t(wg[cols, near], nb[:, near])
            uacc[cols] = dot_t(wu[cols, near], nb[:, near])
        for item in BESIDE[1 + g]:
            relay(*item)
    arrived(("g1",), gains.at[0])

    def send_a(t, c0, cn):
        go(("ax", t), ag.at[row, pl.ds(t * CHUNK, CHUNK), pl.ds(c0, cn)], far)

    for i, (items, relays) in enumerate(PASSES):
        with jax.named_scope(f"norm_pass#{i}"):
            for item in items:
                norm_slice(far_row, slice_of(item))
            arrived(("xf", i), xg.at[0, :, pl.ds(0, len(items) * SLICE)])
            for item in items:
                norm_slice(fsib_row, slice_of(item))
        where = [pl.ds(pl.multiple_of(b * width + slice_of(item) * SLICE, SLICE), SLICE)
                 for item in items for b in (far_row, fsib_row)]

        def product(w, cols):
            return dot_t(jnp.concatenate([w[cols, k] for k in where], axis=1), jnp.concatenate([nb[:, k] for k in where], axis=1))

        if i < len(PASSES) - 1:
            for g, (c0, cn) in enumerate(WIDE):
                cols = slice(c0, c0 + cn)
                with jax.named_scope(f"gu_pass#{i}#{g}"):
                    gate, upv = product(wg, cols), product(wu, cols)
                    gacc[cols] += gate
                    uacc[cols] += upv
                for item in relays[g]:
                    relay(*item)
            continue
        for g, (c0, cn) in enumerate(GROUPS):
            with jax.named_scope(f"gu_last#{g}"):
                cols = slice(c0, c0 + cn)
                gate = gacc[cols] + product(wg, cols)
                upv = uacc[cols] + product(wu, cols)
                ag[row, :, cols] = (jax.nn.silu(gate) * upv).astype(BF16).T
            sent_cn = cn if c0 + cn < ff else wide - c0
            for t in SPLIT_CHUNKS:
                send_a(t, c0, sent_cn)
            go(("as",), ag.at[row, :, pl.ds(c0, sent_cn)], sib)
    for t in range(CHUNKS):
        if t not in SPLIT_CHUNKS:
            send_a(t, 0, wide)

    @scoped
    def forward(t):
        blk = ag.at[far_row, pl.ds(t * CHUNK, CHUNK)]
        arrived(("ax", t), blk)
        go(("af", t), blk, sib)

    loaded(("wd",), wd)
    with jax.named_scope("down_own"):
        acc[...] = dot(ag[row, :, :ff], wd[row])
    with jax.named_scope("down_sib"):
        arrived(("as",), ag.at[sib_row])
        acc[...] += dot(ag[sib_row, :, :ff], wd[sib_row])

    def halves(t):
        t0, tn = t * CHUNK, CHUNK
        hn = tn // 2
        return (pl.ds(pl.multiple_of(t0 + y * hn, hn), hn), pl.ds(pl.multiple_of(t0 + (1 - y) * hn, hn), hn),
                pl.ds(t0 // 2, hn))

    @scoped
    def down_far(t):
        rows = slice(t * CHUNK, (t + 1) * CHUNK)
        acc[rows] += dot(ag[far_row, rows, :ff], wd[far_row])

    def column_parts(t):
        n = LATE_PARTS if t == CHUNKS - 1 else 1
        return [pl.ds(i * (width // n), width // n) for i in range(n)]

    @scoped
    def down_fsib(t):
        rows = slice(t * CHUNK, (t + 1) * CHUNK)
        arrived(("af", t), ag.at[fsib_row, pl.ds(t * CHUNK, CHUNK)])
        _, other, packed = halves(t)
        for i, cols in enumerate(column_parts(t)):
            acc[rows, cols] += dot(ag[fsib_row, rows, :ff], wd[fsib_row, :, cols])
            go(("rs", t, i), acc.at[other, cols], up, rbuf.at[packed, cols])

    @scoped
    def combine(t):
        mine, _, packed = halves(t)
        for i, cols in enumerate(column_parts(t)):
            arrived(("rs", t, i), rbuf.at[packed, cols])
            xn[row, mine, cols] = (xg[row, mine, cols].astype(F32) + (acc[mine, cols] + rbuf[packed, cols])).astype(BF16)
            blk = xn.at[row, mine, cols]
            targets = ([("d", diag)] if DIAGONAL[t] == "d" else []) + [("x", far), ("s", sib)]
            for tag, dev in targets:
                go(("xn", tag, t), blk, dev)

    @scoped
    def send_up(t):
        mine, _, _ = halves(t)
        go(("xn", "y", t), xn.at[row, mine], up)

    @scoped
    def collect(tag, t):
        mine, other, _ = halves(t)
        r, rows = {"y": (row, other), "x": (far_row, mine), "d": (far_row, other)}[tag]
        blk = xn.at[r, rows]
        arrived(("xn", tag, t), blk)
        if (tag, DIAGONAL[t]) in (("y", "x"), ("x", "y")):
            go(("xn", "d", t), blk, far if tag == "y" else up)
        go(("xn", "s", t), blk, sib)

    @scoped
    def finish(t):
        t0, tn = t * CHUNK, CHUNK
        arrived(("xn", "s", t), xn.at[0, pl.ds(0, 2 * CHUNK)])
        res[pl.ds(t0, tn)] = xn[row, pl.ds(t0, tn)]

        def step(i, carry):
            rows = pl.ds(pl.multiple_of(t0 + i * 16, 16), 16)
            blocks = [xn[b, rows].astype(F32) for b in range(4)]
            total = sum(jnp.sum(v * v, axis=1, keepdims=True) for v in blocks)
            r = lax.rsqrt(total / hidden + NORM_EPS)
            for b in range(4):
                nb[rows, b * width:(b + 1) * width] = (blocks[b] * r * gains[b, 1]).astype(BF16)
            return carry
        lax.fori_loop(0, tn // 16, step, 0, unroll=True)

    @scoped
    def project(i):
        if i == 0:
            loaded(("wq",), wq)
        part = wq.shape[1] // 3
        cols = slice(i * part, (i + 1) * part)
        out[:, cols] = dot(nb[:CUT * CHUNK], wq[:, cols]).astype(BF16)

    arrived(("g2",), gains.at[0])
    steps = {"fwd": forward, "dfar": down_far, "dfs": down_fsib, "comb": combine, "sy": send_up, "cy": functools.partial(collect, "y"),
             "cx": functools.partial(collect, "x"), "cd": functools.partial(collect, "d"), "fin": finish, "proj": project}
    for name in STEPS:
        steps[name[:-1]](int(name[-1]))
    with jax.named_scope("drain"):
        pltpu.make_async_copy(sq.at[pl.ds(0, 3)], sq.at[pl.ds(0, 3)], send_sem.at[1]).wait()
        tiles = sum(sent) // (16 * 128 * 2)
        deep = max(d for d in range(1, ff // 16 + 1) if tiles % d == 0)
        like = wg.at[pl.ds(0, deep * 16), pl.ds(0, tiles // deep * 128)]
        pltpu.make_async_copy(like, like, send_sem.at[0]).wait()


def last_kernel(res, first, nb, wq, res_hbm, qkv_hbm, out, sem):
    t0, part = CUT * CHUNK, wq.shape[1] // 2
    copies = [pltpu.make_async_copy(res, res_hbm, sem.at[0]),
              pltpu.make_async_copy(first, qkv_hbm.at[pl.ds(0, t0)], sem.at[1])]
    for c in copies:
        c.start()
    for i in range(2):
        cols = pl.ds(i * part, part)
        out[:, cols] = dot(nb[t0:], wq[:, cols]).astype(BF16)
        c = pltpu.make_async_copy(out.at[:, cols], qkv_hbm.at[pl.ds(t0, out.shape[0]), cols], sem.at[2 + i])
        c.start()
        copies.append(c)
    for c in copies:
        c.wait()


def solution(mesh):
    def per_device(residual, gain_mlp, gain_attn, w_gate, w_up, w_down, w_qkv):
        tokens, width = residual.shape
        ff = w_gate.shape[1]
        qkv = w_qkv.shape[1]
        hidden = width * 4
        any_spec = pl.BlockSpec(memory_space=pl.ANY)
        vmem_spec = pl.BlockSpec(memory_space=pltpu.VMEM)
        held = pl.pallas_call(
            functools.partial(kernel, tokens, width, ff, Names(), Names()),
            out_shape=(pltpu.VMEM((tokens, width), BF16), pltpu.VMEM((CUT * CHUNK, qkv), BF16),
                       pltpu.VMEM((tokens, hidden), BF16), pltpu.VMEM((hidden, qkv), BF16)),
            in_specs=[any_spec] * 7,
            out_specs=(vmem_spec,) * 4,
            scratch_shapes=[
                pltpu.VMEM((4, tokens, width), BF16),
                pltpu.VMEM((ff, hidden), BF16),
                pltpu.VMEM((ff, hidden), BF16),
                pltpu.VMEM((4, ff, width), BF16),
                pltpu.VMEM((4, tokens, (ff + 127) // 128 * 128), BF16),
                pltpu.VMEM((tokens, width), F32),
                pltpu.VMEM((tokens // 2, width), F32),
                pltpu.VMEM((4, tokens, width), BF16),
                pltpu.VMEM((4, 2, 1, width), F32),
                pltpu.VMEM((4, 1, tokens), F32),
                pltpu.VMEM((tokens, 128), F32),
                pltpu.VMEM((ff, tokens), F32),
                pltpu.VMEM((ff, tokens), F32),
                pltpu.SemaphoreType.DMA((2,)),
                pltpu.SemaphoreType.DMA((49,)),
                pltpu.SemaphoreType.DMA((9,)),
            ],
            compiler_params=pltpu.CompilerParams(collective_id=0, has_side_effects=True, vmem_limit_bytes=50_000_000),
            name="block",
        )(residual, gain_mlp.reshape(1, width), gain_attn.reshape(1, width), w_gate.T, w_up.T, w_down, w_qkv)
        return pl.pallas_call(
            last_kernel,
            out_shape=(jax.ShapeDtypeStruct((tokens, width), BF16), jax.ShapeDtypeStruct((tokens, qkv), BF16)),
            in_specs=[vmem_spec] * 4,
            out_specs=(any_spec,) * 2,
            scratch_shapes=[pltpu.VMEM((tokens - CUT * CHUNK, qkv), BF16), pltpu.SemaphoreType.DMA((4,))],
            compiler_params=pltpu.CompilerParams(vmem_limit_bytes=16_000_000),
            name="last",
        )(*(pltpu.with_memory_space_constraint(v, pltpu.VMEM) for v in held))

    return jax.shard_map(
        per_device, mesh=mesh,
        in_specs=(P('data', 'row'), P('row'), P('row'), P(None, ('col', 'row')), P(None, ('col', 'row')),
                  P('col', 'row'), P(None, ('col', 'row'))),
        out_specs=(P('data', 'row'), P('data', ('col', 'row'))), check_vma=False)
```

```python
import functools
import math

import jax
import jax.numpy as jnp
from jax import lax
from jax.experimental import pallas as pl
from jax.experimental.pallas import tpu as pltpu
from jax.sharding import PartitionSpec as P

NORM_EPS = 1e-6
MESH = pl.DeviceIdType.MESH
F32, BF16 = jnp.float32, jnp.bfloat16

SLICE = 128
RELAYED, DIRECT = 3, 5
NEAR = ((0, 352), (352, 336), (688, 352), (1040, 336))
WIDE = ((0, 688), (688, 688))
GROUPS = ((0, 384), (384, 384), (768, 384), (1152, 224))
BESIDE = ((("d", 0, 0),), (("d", 0, 1),), (("d", 1, 0),), (("d", 1, 1), ("d", 2, 0)), (("d", 2, 1), ("r", 0, 0)))
PASSES = (((("d", 0), ("d", 1)), ((("r", 0, 1),), (("r", 1, 0), ("d", 3, None)))),
          ((("d", 2), ("r", 0)), ((("r", 1, 1),), (("d", 4, None), ("r", 2, 0), ("r", 2, 1)))),
          ((("d", 3), ("r", 1)), ((), ())),
          ((("d", 4), ("r", 2)), ()))
CHUNK, CHUNKS = 32, 8
SPLIT_CHUNKS = (0,)
DIAGONAL = "xxxxyxyd"
LATE_PARTS = 1
CUT = 4
STEPS = (
    "fwd0", "dfar0", "dfs0", "fwd1", "dfar1", "dfs1", "fwd2", "dfar2", "dfs2", "comb0", "sy0", "fwd3",
    "dfar3", "dfs3", "comb1", "sy1", "fwd4", "dfar4", "dfs4", "comb2", "sy2", "fwd5", "dfar5", "cy0",
    "dfs5", "comb3", "sy3", "fwd6", "dfar6", "cy1", "dfs6", "fwd7", "comb4", "sy4", "dfar7", "cx0",
    "cy2", "dfs7", "cx1", "cx2", "comb5", "sy5", "cd0", "cy3", "cx3", "fin0", "cd1", "comb6",
    "sy6", "cx4", "cy4", "fin1", "cd2", "cx5", "comb7", "sy7", "fin2", "cd3", "cy5", "cx6",
    "cy6", "fin3", "cd4", "proj0", "proj1", "cy7", "cx7", "fin4", "cd5", "cd6", "cd7", "proj2",
    "fin5", "fin6", "fin7",
)
W_PARTS = 8


def dot(a, b):
    return jnp.dot(a, b, preferred_element_type=F32)


def dot_t(a, b):
    return lax.dot_general(a, b, (((1,), (1,)), ((), ())), preferred_element_type=F32)


def scoped(fn):
    @functools.wraps(fn)
    def run(*args):
        with jax.named_scope("#".join([fn.__name__] + [str(a) for a in args])):
            return fn(*args)
    return run


class Names:
    def __init__(self):
        self.table = {}

    def __call__(self, *key):
        return self.table.setdefault(earlier(key), len(self.table))


def earlier(key):
    if key[0] != "xn":
        return key
    tag, t = key[1:]
    if tag == "x":
        return ("xx",) + ((t // 2, t % 2) if t < 2 * RELAYED else (t - RELAYED, None))
    if tag == "y":
        return ("xy", t // 2, t % 2) if t < 2 * RELAYED else ("rs", t - 2 * RELAYED, 0)
    if tag == "s":
        return ("as",) if t == 0 else ("af", t - 1)
    return ("xf", t) if t < len(PASSES) else (("sq",), ("xs",), ("gs",), ("g1",))[t - len(PASSES)]


def kernel(tokens, width, ff, names, local_names,
           x_hbm, g1_hbm, g2_hbm, wg_hbm, wu_hbm, wd_hbm, wq_hbm, res, out, nb, wq,
           xg, wg, wu, wd, ag, acc, rbuf, xn, gains, sq, scale, gacc, uacc, send_sem, recv_sem, loc_sem):
    data, y, row = lax.axis_index("data"), lax.axis_index("col"), lax.axis_index("row")
    cx = row // 2
    core = row - cx * 2
    sib_row = cx * 2 + 1 - core
    far_row = (1 - cx) * 2 + core
    fsib_row = (1 - cx) * 2 + 1 - core
    sib, far, fsib = (data, y, sib_row), (data, y, far_row), (data, y, fsib_row)
    up, diag = (data, 1 - y, row), (data, 1 - y, far_row)
    hidden = width * 4
    wide = ag.shape[2]
    slices = width // SLICE

    def remote(key, src, dst, dev):
        return pltpu.make_async_remote_copy(src_ref=src, dst_ref=dst, send_sem=send_sem.at[1 if key[0] == "sq" else 0], recv_sem=recv_sem.at[names(*key)],
                                            device_id=dev, device_id_type=MESH)

    def local(key, src, dst):
        return pltpu.make_async_copy(src, dst, loc_sem.at[local_names(*key)])

    def arrived(key, like):
        pltpu.make_async_copy(like, like, recv_sem.at[names(*key)]).wait()

    def loaded(key, like):
        pltpu.make_async_copy(like, like, loc_sem.at[local_names(*key)]).wait()

    sent = []

    def go(key, ref, dev, dst=None):
        copy = remote(key, ref, ref if dst is None else dst, dev)
        copy.start()
        if key[0] != "sq":
            sent.append(math.prod(ref.shape) * jnp.dtype(ref.dtype).itemsize)
        return copy

    own = [local(("x",), x_hbm, xg.at[row]), local(("g1",), g1_hbm, gains.at[row, 0]), local(("g2",), g2_hbm, gains.at[row, 1])]
    for c in own:
        c.start()
    for g, (c0, cn) in enumerate(NEAR):
        for src, dst in ((wg_hbm, wg), (wu_hbm, wu)):
            local(("w", g), src.at[pl.ds(c0, cn)], dst.at[pl.ds(c0, cn)]).start()
    for i in range(4):
        local(("wd",), wd_hbm.at[pl.ds(i * ff, ff)], wd.at[i]).start()
    part = hidden // W_PARTS
    for i in range(W_PARTS):
        local(("wq",), wq_hbm.at[pl.ds(i * part, part)], wq.at[pl.ds(i * part, part)]).start()

    barrier = pltpu.get_barrier_semaphore()
    for dev in (sib, far, fsib, up, diag):
        pl.semaphore_signal(barrier, inc=1, device_id=dev, device_id_type=MESH)

    with jax.named_scope("own"):
        if wide > ff:
            ag[row, :, ff:] = jnp.zeros((tokens, wide - ff), BF16)
        for c in own:
            c.wait()
        part = sum(jnp.square(xg[row, :, i:i + 128].astype(F32)) for i in range(0, width, 128)).T
        sq[row] = jnp.sum(part, axis=0, keepdims=True)
    with jax.named_scope("barrier"):
        pl.semaphore_wait(barrier, 5)

    def cut(k):
        return pl.ds(pl.multiple_of(k * SLICE, SLICE), SLICE)

    def direct_slice(p):
        return y * (slices - RELAYED) + p if p < RELAYED else p

    def relayed_slice(q):
        return (1 - y) * (slices - RELAYED) + q

    def slice_of(item):
        return direct_slice(item[1]) if item[0] == "d" else relayed_slice(item[1])

    def parts(item):
        return (0, 1) if item[0] == "r" or item[1] < RELAYED else (None,)

    def x_block(b, item):
        toks = slice(None) if item[2] is None else pl.ds(item[2] * (tokens // 2), tokens // 2)
        return xg.at[b, toks, cut(slice_of(item))]

    x_in = {}
    pass_of = {item: i for i, (items, _) in enumerate(PASSES) for item in items}

    def send_x(p):
        for h in parts(("d", p)):
            x_in["d", p, h] = go(("xx", p, h), x_block(row, ("d", p, h)), far)

    for dev in (far, fsib, sib):
        go(("sq",), sq.at[row], dev)
    x_sib = go(("xs",), xg.at[row], sib)
    go(("gs",), gains.at[row], sib)
    send_x(0)
    for dev in (far, fsib):
        go(("g1",), gains.at[row, 0], dev)
    for p in range(1, DIRECT):
        send_x(p)
    for dev in (far, fsib):
        go(("g2",), gains.at[row, 1], dev)

    def norm_slice(b, k):
        cols = pl.ds(pl.multiple_of(b * width + k * SLICE, SLICE), SLICE)
        nb[:, cols] = (xg[b, :, cut(k)].astype(F32) * scale[...] * gains[b, 0, :, cut(k)]).astype(BF16)

    def norm_block(b):
        def step(k, carry):
            norm_slice(b, k)
            return carry
        lax.fori_loop(0, slices, step, 0)

    @scoped
    def relay(*item):
        x_in[item].wait_recv()
        blk = x_block(far_row, item)
        kind, p, h = item
        if kind == "d" and p < RELAYED:
            x_in["r", p, h] = go(("xy", p, h), blk, up)
        go(("xf", pass_of[kind, p]), blk, sib)

    with jax.named_scope("stats"):
        arrived(("sq",), sq.at[pl.ds(0, 3)])
        mean = (sq[0] + sq[1] + sq[2] + sq[3]) / hidden
        scale[...] = jnp.broadcast_to(lax.rsqrt(mean + NORM_EPS), (128, tokens)).T
    with jax.named_scope("norm_own"):
        norm_block(row)
    with jax.named_scope("norm_sib"):
        x_sib.wait_recv()
        arrived(("gs",), gains.at[0])
        norm_block(sib_row)

    near = pl.ds(pl.multiple_of(cx * 2 * width, 2 * width), 2 * width)
    for item in BESIDE[0]:
        relay(*item)
    for g, (c0, cn) in enumerate(NEAR):
        cols = slice(c0, c0 + cn)
        with jax.named_scope(f"gu_near#{g}"):
            loaded(("w", g), wg.at[pl.ds(0, 2 * cn)])
            gacc[cols] = dot_t(wg[cols, near], nb[:, near])
            uacc[cols] = dot_t(wu[cols, near], nb[:, near])
        for item in BESIDE[1 + g]:
            relay(*item)
    arrived(("g1",), gains.at[0])

    def send_a(t, c0, cn):
        go(("ax", t), ag.at[row, pl.ds(t * CHUNK, CHUNK), pl.ds(c0, cn)], far)

    for i, (items, relays) in enumerate(PASSES):
        with jax.named_scope(f"norm_pass#{i}"):
            for item in items:
                norm_slice(far_row, slice_of(item))
            arrived(("xf", i), xg.at[0, :, pl.ds(0, len(items) * SLICE)])
            for item in items:
                norm_slice(fsib_row, slice_of(item))
        where = [pl.ds(pl.multiple_of(b * width + slice_of(item) * SLICE, SLICE), SLICE)
                 for item in items for b in (far_row, fsib_row)]

        def product(w, cols):
            return dot_t(jnp.concatenate([w[cols, k] for k in where], axis=1), jnp.concatenate([nb[:, k] for k in where], axis=1))

        if i < len(PASSES) - 1:
            for g, (c0, cn) in enumerate(WIDE):
                cols = slice(c0, c0 + cn)
                with jax.named_scope(f"gu_pass#{i}#{g}"):
                    gate, upv = product(wg, cols), product(wu, cols)
                    gacc[cols] += gate
                    uacc[cols] += upv
                for item in relays[g]:
                    relay(*item)
            continue
        for g, (c0, cn) in enumerate(GROUPS):
            with jax.named_scope(f"gu_last#{g}"):
                cols = slice(c0, c0 + cn)
                gate = gacc[cols] + product(wg, cols)
                upv = uacc[cols] + product(wu, cols)
                ag[row, :, cols] = (jax.nn.silu(gate) * upv).astype(BF16).T
            sent_cn = cn if c0 + cn < ff else wide - c0
            for t in SPLIT_CHUNKS:
                send_a(t, c0, sent_cn)
            go(("as",), ag.at[row, :, pl.ds(c0, sent_cn)], sib)
    for t in range(CHUNKS):
        if t not in SPLIT_CHUNKS:
            send_a(t, 0, wide)

    @scoped
    def forward(t):
        blk = ag.at[far_row, pl.ds(t * CHUNK, CHUNK)]
        arrived(("ax", t), blk)
        go(("af", t), blk, sib)

    loaded(("wd",), wd)
    with jax.named_scope("down_own"):
        acc[...] = dot(ag[row, :, :ff], wd[row])
    with jax.named_scope("down_sib"):
        arrived(("as",), ag.at[sib_row])
        acc[...] += dot(ag[sib_row, :, :ff], wd[sib_row])

    def halves(t):
        t0, tn = t * CHUNK, CHUNK
        hn = tn // 2
        return (pl.ds(pl.multiple_of(t0 + y * hn, hn), hn), pl.ds(pl.multiple_of(t0 + (1 - y) * hn, hn), hn),
                pl.ds(t0 // 2, hn))

    @scoped
    def down_far(t):
        rows = slice(t * CHUNK, (t + 1) * CHUNK)
        acc[rows] += dot(ag[far_row, rows, :ff], wd[far_row])

    def column_parts(t):
        n = LATE_PARTS if t == CHUNKS - 1 else 1
        return [pl.ds(i * (width // n), width // n) for i in range(n)]

    @scoped
    def down_fsib(t):
        rows = slice(t * CHUNK, (t + 1) * CHUNK)
        arrived(("af", t), ag.at[fsib_row, pl.ds(t * CHUNK, CHUNK)])
        _, other, packed = halves(t)
        for i, cols in enumerate(column_parts(t)):
            acc[rows, cols] += dot(ag[fsib_row, rows, :ff], wd[fsib_row, :, cols])
            go(("rs", t, i), acc.at[other, cols], up, rbuf.at[packed, cols])

    @scoped
    def combine(t):
        mine, _, packed = halves(t)
        for i, cols in enumerate(column_parts(t)):
            arrived(("rs", t, i), rbuf.at[packed, cols])
            xn[row, mine, cols] = (xg[row, mine, cols].astype(F32) + (acc[mine, cols] + rbuf[packed, cols])).astype(BF16)
            blk = xn.at[row, mine, cols]
            targets = ([("d", diag)] if DIAGONAL[t] == "d" else []) + [("x", far), ("s", sib)]
            for tag, dev in targets:
                go(("xn", tag, t), blk, dev)

    @scoped
    def send_up(t):
        mine, _, _ = halves(t)
        go(("xn", "y", t), xn.at[row, mine], up)

    @scoped
    def collect(tag, t):
        mine, other, _ = halves(t)
        r, rows = {"y": (row, other), "x": (far_row, mine), "d": (far_row, other)}[tag]
        blk = xn.at[r, rows]
        arrived(("xn", tag, t), blk)
        if (tag, DIAGONAL[t]) in (("y", "x"), ("x", "y")):
            go(("xn", "d", t), blk, far if tag == "y" else up)
        go(("xn", "s", t), blk, sib)

    @scoped
    def finish(t):
        t0, tn = t * CHUNK, CHUNK
        arrived(("xn", "s", t), xn.at[0, pl.ds(0, 2 * CHUNK)])
        res[pl.ds(t0, tn)] = xn[row, pl.ds(t0, tn)]

        def step(i, carry):
            rows = pl.ds(pl.multiple_of(t0 + i * 16, 16), 16)
            blocks = [xn[b, rows].astype(F32) for b in range(4)]
            total = sum(jnp.sum(v * v, axis=1, keepdims=True) for v in blocks)
            r = lax.rsqrt(total / hidden + NORM_EPS)
            for b in range(4):
                nb[rows, b * width:(b + 1) * width] = (blocks[b] * r * gains[b, 1]).astype(BF16)
            return carry
        lax.fori_loop(0, tn // 16, step, 0, unroll=True)

    @scoped
    def project(i):
        if i == 0:
            loaded(("wq",), wq)
        part = wq.shape[1] // 3
        cols = slice(i * part, (i + 1) * part)
        out[:, cols] = dot(nb[:CUT * CHUNK], wq[:, cols]).astype(BF16)

    arrived(("g2",), gains.at[0])
    steps = {"fwd": forward, "dfar": down_far, "dfs": down_fsib, "comb": combine, "sy": send_up, "cy": functools.partial(collect, "y"),
             "cx": functools.partial(collect, "x"), "cd": functools.partial(collect, "d"), "fin": finish, "proj": project}
    for name in STEPS:
        steps[name[:-1]](int(name[-1]))
    with jax.named_scope("drain"):
        pltpu.make_async_copy(sq.at[pl.ds(0, 3)], sq.at[pl.ds(0, 3)], send_sem.at[1]).wait()
        tiles = sum(sent) // (16 * 128 * 2)
        deep = max(d for d in range(1, ff // 16 + 1) if tiles % d == 0)
        like = wg.at[pl.ds(0, deep * 16), pl.ds(0, tiles // deep * 128)]
        pltpu.make_async_copy(like, like, send_sem.at[0]).wait()


def last_kernel(res, first, nb, wq, res_hbm, qkv_hbm, out, sem):
    t0, part = CUT * CHUNK, wq.shape[1] // 2
    copies = [pltpu.make_async_copy(res, res_hbm, sem.at[0]),
              pltpu.make_async_copy(first, qkv_hbm.at[pl.ds(0, t0)], sem.at[1])]
    for c in copies:
        c.start()
    for i in range(2):
        cols = pl.ds(i * part, part)
        out[:, cols] = dot(nb[t0:], wq[:, cols]).astype(BF16)
        c = pltpu.make_async_copy(out.at[:, cols], qkv_hbm.at[pl.ds(t0, out.shape[0]), cols], sem.at[2 + i])
        c.start()
        copies.append(c)
    for c in copies:
        c.wait()


def solution(mesh):
    def per_device(residual, gain_mlp, gain_attn, w_gate, w_up, w_down, w_qkv):
        tokens, width = residual.shape
        ff = w_gate.shape[1]
        qkv = w_qkv.shape[1]
        hidden = width * 4
        any_spec = pl.BlockSpec(memory_space=pl.ANY)
        vmem_spec = pl.BlockSpec(memory_space=pltpu.VMEM)
        held = pl.pallas_call(
            functools.partial(kernel, tokens, width, ff, Names(), Names()),
            out_shape=(pltpu.VMEM((tokens, width), BF16), pltpu.VMEM((CUT * CHUNK, qkv), BF16),
                       pltpu.VMEM((tokens, hidden), BF16), pltpu.VMEM((hidden, qkv), BF16)),
            in_specs=[any_spec] * 7,
            out_specs=(vmem_spec,) * 4,
            scratch_shapes=[
                pltpu.VMEM((4, tokens, width), BF16),
                pltpu.VMEM((ff, hidden), BF16),
                pltpu.VMEM((ff, hidden), BF16),
                pltpu.VMEM((4, ff, width), BF16),
                pltpu.VMEM((4, tokens, (ff + 127) // 128 * 128), BF16),
                pltpu.VMEM((tokens, width), F32),
                pltpu.VMEM((tokens // 2, width), F32),
                pltpu.VMEM((4, tokens, width), BF16),
                pltpu.VMEM((4, 2, 1, width), F32),
                pltpu.VMEM((4, 1, tokens), F32),
                pltpu.VMEM((tokens, 128), F32),
                pltpu.VMEM((ff, tokens), F32),
                pltpu.VMEM((ff, tokens), F32),
                pltpu.SemaphoreType.DMA((2,)),
                pltpu.SemaphoreType.DMA((49,)),
                pltpu.SemaphoreType.DMA((9,)),
            ],
            compiler_params=pltpu.CompilerParams(collective_id=0, has_side_effects=True, vmem_limit_bytes=50_000_000),
            name="block",
        )(residual, gain_mlp.reshape(1, width), gain_attn.reshape(1, width), w_gate.T, w_up.T, w_down, w_qkv)
        return pl.pallas_call(
            last_kernel,
            out_shape=(jax.ShapeDtypeStruct((tokens, width), BF16), jax.ShapeDtypeStruct((tokens, qkv), BF16)),
            in_specs=[vmem_spec] * 4,
            out_specs=(any_spec,) * 2,
            scratch_shapes=[pltpu.VMEM((tokens - CUT * CHUNK, qkv), BF16), pltpu.SemaphoreType.DMA((4,))],
            compiler_params=pltpu.CompilerParams(vmem_limit_bytes=16_000_000),
            name="last",
        )(*(pltpu.with_memory_space_constraint(v, pltpu.VMEM) for v in held))

    return jax.shard_map(
        per_device, mesh=mesh,
        in_specs=(P('data', 'row'), P('row'), P('row'), P(None, ('col', 'row')), P(None, ('col', 'row')),
                  P('col', 'row'), P(None, ('col', 'row'))),
        out_specs=(P('data', 'row'), P('data', ('col', 'row'))), check_vma=False)
```

```python
import functools
import math

import jax
import jax.numpy as jnp
from jax import lax
from jax.experimental import pallas as pl
from jax.experimental.pallas import tpu as pltpu
from jax.sharding import PartitionSpec as P

NORM_EPS = 1e-6
MESH = pl.DeviceIdType.MESH
F32, BF16 = jnp.float32, jnp.bfloat16

SLICE = 128
RELAYED, DIRECT = 3, 5
NEAR = ((0, 352), (352, 336), (688, 352), (1040, 336))
WIDE = ((0, 688), (688, 688))
GROUPS = ((0, 384), (384, 384), (768, 384), (1152, 224))
BESIDE = ((("d", 0, 0),), (("d", 0, 1),), (("d", 1, 0),), (("d", 1, 1), ("d", 2, 0)), (("d", 2, 1), ("r", 0, 0)))
PASSES = (((("d", 0), ("d", 1)), ((("r", 0, 1),), (("r", 1, 0), ("d", 3, None)))),
          ((("d", 2), ("r", 0)), ((("r", 1, 1),), (("d", 4, None), ("r", 2, 0), ("r", 2, 1)))),
          ((("d", 3), ("r", 1)), ((), ())),
          ((("d", 4), ("r", 2)), ()))
CHUNK, CHUNKS = 32, 8
SPLIT_CHUNKS = (0,)
DIAGONAL = "xxxxyxyd"
LATE_PARTS = 1
CUT = 4
STEPS = (
    "fwd0", "dfar0", "dfs0", "fwd1", "dfar1", "dfs1", "fwd2", "dfar2", "dfs2", "comb0", "sy0", "fwd3",
    "dfar3", "dfs3", "comb1", "sy1", "fwd4", "dfar4", "dfs4", "comb2", "sy2", "fwd5", "dfar5", "cy0",
    "dfs5", "comb3", "sy3", "fwd6", "dfar6", "cy1", "dfs6", "fwd7", "comb4", "sy4", "dfar7", "cx0",
    "cy2", "dfs7", "cx1", "cx2", "comb5", "sy5", "cd0", "cy3", "cx3", "fin0", "cd1", "comb6",
    "sy6", "cx4", "cy4", "fin1", "cd2", "cx5", "comb7", "sy7", "fin2", "cd3", "cy5", "cx6",
    "cy6", "fin3", "cd4", "proj0", "proj1", "cy7", "cx7", "fin4", "cd5", "cd6", "cd7", "proj2",
    "fin5", "fin6", "fin7",
)
W_PARTS = 8


def dot(a, b):
    return jnp.dot(a, b, preferred_element_type=F32)


def dot_t(a, b):
    return lax.dot_general(a, b, (((1,), (1,)), ((), ())), preferred_element_type=F32)


def scoped(fn):
    @functools.wraps(fn)
    def run(*args):
        with jax.named_scope("#".join([fn.__name__] + [str(a) for a in args])):
            return fn(*args)
    return run


class Names:
    def __init__(self):
        self.table = {}

    def __call__(self, *key):
        return self.table.setdefault(earlier(key), len(self.table))


def earlier(key):
    if key[0] != "xn":
        return key
    tag, t = key[1:]
    if tag == "x":
        return ("xx",) + ((t // 2, t % 2) if t < 2 * RELAYED else (t - RELAYED, None))
    if tag == "y":
        return ("xy", t // 2, t % 2) if t < 2 * RELAYED else ("rs", t - 2 * RELAYED, 0)
    if tag == "s":
        return ("as",) if t == 0 else ("af", t - 1)
    return ("xf", t) if t < len(PASSES) else (("sq",), ("xs",), ("gs",), ("g1",))[t - len(PASSES)]


def kernel(tokens, width, ff, names, local_names,
           x_hbm, g1_hbm, g2_hbm, wg_hbm, wu_hbm, wd_hbm, wq_hbm, res, out, nb, wq,
           xg, wg, wu, wd, ag, acc, rbuf, xn, gains, sq, scale, gacc, uacc, send_sem, recv_sem, loc_sem):
    data, y, row = lax.axis_index("data"), lax.axis_index("col"), lax.axis_index("row")
    cx = row // 2
    core = row - cx * 2
    sib_row = cx * 2 + 1 - core
    far_row = (1 - cx) * 2 + core
    fsib_row = (1 - cx) * 2 + 1 - core
    sib, far, fsib = (data, y, sib_row), (data, y, far_row), (data, y, fsib_row)
    up, diag = (data, 1 - y, row), (data, 1 - y, far_row)
    hidden = width * 4
    wide = ag.shape[2]
    slices = width // SLICE

    def remote(key, src, dst, dev):
        return pltpu.make_async_remote_copy(src_ref=src, dst_ref=dst, send_sem=send_sem.at[1 if key[0] == "sq" else 0], recv_sem=recv_sem.at[names(*key)],
                                            device_id=dev, device_id_type=MESH)

    def local(key, src, dst):
        return pltpu.make_async_copy(src, dst, loc_sem.at[local_names(*key)])

    def arrived(key, like):
        pltpu.make_async_copy(like, like, recv_sem.at[names(*key)]).wait()

    def loaded(key, like):
        pltpu.make_async_copy(like, like, loc_sem.at[local_names(*key)]).wait()

    sent = []

    def go(key, ref, dev, dst=None):
        copy = remote(key, ref, ref if dst is None else dst, dev)
        copy.start()
        if key[0] != "sq":
            sent.append(math.prod(ref.shape) * jnp.dtype(ref.dtype).itemsize)
        return copy

    own = [local(("x",), x_hbm, xg.at[row]), local(("g1",), g1_hbm, gains.at[row, 0]), local(("g2",), g2_hbm, gains.at[row, 1])]
    for c in own:
        c.start()
    near = pl.ds(pl.multiple_of(cx * 2 * width, 2 * width), 2 * width)
    away = pl.ds(pl.multiple_of((1 - cx) * 2 * width, 2 * width), 2 * width)
    for part in (near, away):
        for g, (c0, cn) in enumerate(NEAR):
            for src, dst in ((wg_hbm, wg), (wu_hbm, wu)):
                key = ("w", g) if part is near else ("w", len(NEAR))
                local(key, src.at[pl.ds(c0, cn), part], dst.at[pl.ds(c0, cn), part]).start()
    for i in range(4):
        local(("wd",), wd_hbm.at[pl.ds(i * ff, ff)], wd.at[i]).start()
    part = hidden // W_PARTS
    for i in range(W_PARTS):
        local(("wq",), wq_hbm.at[pl.ds(i * part, part)], wq.at[pl.ds(i * part, part)]).start()

    barrier = pltpu.get_barrier_semaphore()
    for dev in (sib, far, fsib, up, diag):
        pl.semaphore_signal(barrier, inc=1, device_id=dev, device_id_type=MESH)

    with jax.named_scope("own"):
        if wide > ff:
            ag[row, :, ff:] = jnp.zeros((tokens, wide - ff), BF16)
        for c in own:
            c.wait()
        part = sum(jnp.square(xg[row, :, i:i + 128].astype(F32)) for i in range(0, width, 128)).T
        sq[row] = jnp.sum(part, axis=0, keepdims=True)
    with jax.named_scope("barrier"):
        pl.semaphore_wait(barrier, 5)

    def cut(k):
        return pl.ds(pl.multiple_of(k * SLICE, SLICE), SLICE)

    def direct_slice(p):
        return y * (slices - RELAYED) + p if p < RELAYED else p

    def relayed_slice(q):
        return (1 - y) * (slices - RELAYED) + q

    def slice_of(item):
        return direct_slice(item[1]) if item[0] == "d" else relayed_slice(item[1])

    def parts(item):
        return (0, 1) if item[0] == "r" or item[1] < RELAYED else (None,)

    def x_block(b, item):
        toks = slice(None) if item[2] is None else pl.ds(item[2] * (tokens // 2), tokens // 2)
        return xg.at[b, toks, cut(slice_of(item))]

    x_in = {}
    pass_of = {item: i for i, (items, _) in enumerate(PASSES) for item in items}

    def send_x(p):
        for h in parts(("d", p)):
            x_in["d", p, h] = go(("xx", p, h), x_block(row, ("d", p, h)), far)

    for dev in (far, fsib, sib):
        go(("sq",), sq.at[row], dev)
    x_sib = go(("xs",), xg.at[row], sib)
    go(("gs",), gains.at[row], sib)
    send_x(0)
    for dev in (far, fsib):
        go(("g1",), gains.at[row, 0], dev)
    for p in range(1, DIRECT):
        send_x(p)
    for dev in (far, fsib):
        go(("g2",), gains.at[row, 1], dev)

    def norm_slice(b, k):
        cols = pl.ds(pl.multiple_of(b * width + k * SLICE, SLICE), SLICE)
        nb[:, cols] = (xg[b, :, cut(k)].astype(F32) * scale[...] * gains[b, 0, :, cut(k)]).astype(BF16)

    def norm_block(b):
        def step(k, carry):
            norm_slice(b, k)
            return carry
        lax.fori_loop(0, slices, step, 0)

    @scoped
    def relay(*item):
        x_in[item].wait_recv()
        blk = x_block(far_row, item)
        kind, p, h = item
        if kind == "d" and p < RELAYED:
            x_in["r", p, h] = go(("xy", p, h), blk, up)
        go(("xf", pass_of[kind, p]), blk, sib)

    with jax.named_scope("stats"):
        arrived(("sq",), sq.at[pl.ds(0, 3)])
        mean = (sq[0] + sq[1] + sq[2] + sq[3]) / hidden
        scale[...] = jnp.broadcast_to(lax.rsqrt(mean + NORM_EPS), (128, tokens)).T
    with jax.named_scope("norm_own"):
        norm_block(row)
    with jax.named_scope("norm_sib"):
        x_sib.wait_recv()
        arrived(("gs",), gains.at[0])
        norm_block(sib_row)

    for item in BESIDE[0]:
        relay(*item)
    for g, (c0, cn) in enumerate(NEAR):
        cols = slice(c0, c0 + cn)
        with jax.named_scope(f"gu_near#{g}"):
            loaded(("w", g), wg.at[pl.ds(0, cn)])
            gacc[cols] = dot_t(wg[cols, near], nb[:, near])
            uacc[cols] = dot_t(wu[cols, near], nb[:, near])
        for item in BESIDE[1 + g]:
            relay(*item)
    arrived(("g1",), gains.at[0])
    loaded(("w", len(NEAR)), wg)

    def send_a(t, c0, cn):
        go(("ax", t), ag.at[row, pl.ds(t * CHUNK, CHUNK), pl.ds(c0, cn)], far)

    for i, (items, relays) in enumerate(PASSES):
        with jax.named_scope(f"norm_pass#{i}"):
            for item in items:
                norm_slice(far_row, slice_of(item))
            arrived(("xf", i), xg.at[0, :, pl.ds(0, len(items) * SLICE)])
            for item in items:
                norm_slice(fsib_row, slice_of(item))
        where = [pl.ds(pl.multiple_of(b * width + slice_of(item) * SLICE, SLICE), SLICE)
                 for item in items for b in (far_row, fsib_row)]

        def product(w, cols):
            return dot_t(jnp.concatenate([w[cols, k] for k in where], axis=1), jnp.concatenate([nb[:, k] for k in where], axis=1))

        if i < len(PASSES) - 1:
            for g, (c0, cn) in enumerate(WIDE if any(relays) else ((0, ff),)):
                cols = slice(c0, c0 + cn)
                with jax.named_scope(f"gu_pass#{i}#{g}"):
                    gate, upv = product(wg, cols), product(wu, cols)
                    gacc[cols] += gate
                    uacc[cols] += upv
                for item in relays[g]:
                    relay(*item)
            continue
        for g, (c0, cn) in enumerate(GROUPS):
            with jax.named_scope(f"gu_last#{g}"):
                cols = slice(c0, c0 + cn)
                gate = gacc[cols] + product(wg, cols)
                upv = uacc[cols] + product(wu, cols)
                ag[row, :, cols] = (jax.nn.silu(gate) * upv).astype(BF16).T
            sent_cn = cn if c0 + cn < ff else wide - c0
            for t in SPLIT_CHUNKS:
                send_a(t, c0, sent_cn)
            go(("as",), ag.at[row, :, pl.ds(c0, sent_cn)], sib)
    for t in range(CHUNKS):
        if t not in SPLIT_CHUNKS:
            send_a(t, 0, wide)

    @scoped
    def forward(t):
        blk = ag.at[far_row, pl.ds(t * CHUNK, CHUNK)]
        arrived(("ax", t), blk)
        go(("af", t), blk, sib)

    loaded(("wd",), wd)
    with jax.named_scope("down_own"):
        acc[...] = dot(ag[row, :, :ff], wd[row])
    with jax.named_scope("down_sib"):
        arrived(("as",), ag.at[sib_row])
        acc[...] += dot(ag[sib_row, :, :ff], wd[sib_row])

    def halves(t):
        t0, tn = t * CHUNK, CHUNK
        hn = tn // 2
        return (pl.ds(pl.multiple_of(t0 + y * hn, hn), hn), pl.ds(pl.multiple_of(t0 + (1 - y) * hn, hn), hn),
                pl.ds(t0 // 2, hn))

    @scoped
    def down_far(t):
        rows = slice(t * CHUNK, (t + 1) * CHUNK)
        acc[rows] += dot(ag[far_row, rows, :ff], wd[far_row])

    def column_parts(t):
        n = LATE_PARTS if t == CHUNKS - 1 else 1
        return [pl.ds(i * (width // n), width // n) for i in range(n)]

    @scoped
    def down_fsib(t):
        rows = slice(t * CHUNK, (t + 1) * CHUNK)
        arrived(("af", t), ag.at[fsib_row, pl.ds(t * CHUNK, CHUNK)])
        _, other, packed = halves(t)
        for i, cols in enumerate(column_parts(t)):
            acc[rows, cols] += dot(ag[fsib_row, rows, :ff], wd[fsib_row, :, cols])
            go(("rs", t, i), acc.at[other, cols], up, rbuf.at[packed, cols])

    @scoped
    def combine(t):
        mine, _, packed = halves(t)
        for i, cols in enumerate(column_parts(t)):
            arrived(("rs", t, i), rbuf.at[packed, cols])
            xn[row, mine, cols] = (xg[row, mine, cols].astype(F32) + (acc[mine, cols] + rbuf[packed, cols])).astype(BF16)
            blk = xn.at[row, mine, cols]
            targets = ([("d", diag)] if DIAGONAL[t] == "d" else []) + [("x", far), ("s", sib)]
            for tag, dev in targets:
                go(("xn", tag, t), blk, dev)

    @scoped
    def send_up(t):
        mine, _, _ = halves(t)
        go(("xn", "y", t), xn.at[row, mine], up)

    @scoped
    def collect(tag, t):
        mine, other, _ = halves(t)
        r, rows = {"y": (row, other), "x": (far_row, mine), "d": (far_row, other)}[tag]
        blk = xn.at[r, rows]
        arrived(("xn", tag, t), blk)
        if (tag, DIAGONAL[t]) in (("y", "x"), ("x", "y")):
            go(("xn", "d", t), blk, far if tag == "y" else up)
        go(("xn", "s", t), blk, sib)

    @scoped
    def finish(t):
        t0, tn = t * CHUNK, CHUNK
        arrived(("xn", "s", t), xn.at[0, pl.ds(0, 2 * CHUNK)])
        res[pl.ds(t0, tn)] = xn[row, pl.ds(t0, tn)]

        def step(i, carry):
            rows = pl.ds(pl.multiple_of(t0 + i * 16, 16), 16)
            blocks = [xn[b, rows].astype(F32) for b in range(4)]
            total = sum(jnp.sum(v * v, axis=1, keepdims=True) for v in blocks)
            r = lax.rsqrt(total / hidden + NORM_EPS)
            for b in range(4):
                nb[rows, b * width:(b + 1) * width] = (blocks[b] * r * gains[b, 1]).astype(BF16)
            return carry
        lax.fori_loop(0, tn // 16, step, 0, unroll=True)

    @scoped
    def project(i):
        if i == 0:
            loaded(("wq",), wq)
        part = wq.shape[1] // 3
        cols = slice(i * part, (i + 1) * part)
        out[:, cols] = dot(nb[:CUT * CHUNK], wq[:, cols]).astype(BF16)

    arrived(("g2",), gains.at[0])
    steps = {"fwd": forward, "dfar": down_far, "dfs": down_fsib, "comb": combine, "sy": send_up, "cy": functools.partial(collect, "y"),
             "cx": functools.partial(collect, "x"), "cd": functools.partial(collect, "d"), "fin": finish, "proj": project}
    for name in STEPS:
        steps[name[:-1]](int(name[-1]))
    with jax.named_scope("drain"):
        pltpu.make_async_copy(sq.at[pl.ds(0, 3)], sq.at[pl.ds(0, 3)], send_sem.at[1]).wait()
        tiles = sum(sent) // (16 * 128 * 2)
        deep = max(d for d in range(1, ff // 16 + 1) if tiles % d == 0)
        like = wg.at[pl.ds(0, deep * 16), pl.ds(0, tiles // deep * 128)]
        pltpu.make_async_copy(like, like, send_sem.at[0]).wait()


def last_kernel(res, first, nb, wq, res_hbm, qkv_hbm, out, sem):
    t0, part = CUT * CHUNK, wq.shape[1] // 2
    copies = [pltpu.make_async_copy(res, res_hbm, sem.at[0]),
              pltpu.make_async_copy(first, qkv_hbm.at[pl.ds(0, t0)], sem.at[1])]
    for c in copies:
        c.start()
    for i in range(2):
        cols = pl.ds(i * part, part)
        out[:, cols] = dot(nb[t0:], wq[:, cols]).astype(BF16)
        c = pltpu.make_async_copy(out.at[:, cols], qkv_hbm.at[pl.ds(t0, out.shape[0]), cols], sem.at[2 + i])
        c.start()
        copies.append(c)
    for c in copies:
        c.wait()


def solution(mesh):
    def per_device(residual, gain_mlp, gain_attn, w_gate, w_up, w_down, w_qkv):
        tokens, width = residual.shape
        ff = w_gate.shape[1]
        qkv = w_qkv.shape[1]
        hidden = width * 4
        any_spec = pl.BlockSpec(memory_space=pl.ANY)
        vmem_spec = pl.BlockSpec(memory_space=pltpu.VMEM)
        held = pl.pallas_call(
            functools.partial(kernel, tokens, width, ff, Names(), Names()),
            out_shape=(pltpu.VMEM((tokens, width), BF16), pltpu.VMEM((CUT * CHUNK, qkv), BF16),
                       pltpu.VMEM((tokens, hidden), BF16), pltpu.VMEM((hidden, qkv), BF16)),
            in_specs=[any_spec] * 7,
            out_specs=(vmem_spec,) * 4,
            scratch_shapes=[
                pltpu.VMEM((4, tokens, width), BF16),
                pltpu.VMEM((ff, hidden), BF16),
                pltpu.VMEM((ff, hidden), BF16),
                pltpu.VMEM((4, ff, width), BF16),
                pltpu.VMEM((4, tokens, (ff + 127) // 128 * 128), BF16),
                pltpu.VMEM((tokens, width), F32),
                pltpu.VMEM((tokens // 2, width), F32),
                pltpu.VMEM((4, tokens, width), BF16),
                pltpu.VMEM((4, 2, 1, width), F32),
                pltpu.VMEM((4, 1, tokens), F32),
                pltpu.VMEM((tokens, 128), F32),
                pltpu.VMEM((ff, tokens), F32),
                pltpu.VMEM((ff, tokens), F32),
                pltpu.SemaphoreType.DMA((2,)),
                pltpu.SemaphoreType.DMA((49,)),
                pltpu.SemaphoreType.DMA((10,)),
            ],
            compiler_params=pltpu.CompilerParams(collective_id=0, has_side_effects=True, vmem_limit_bytes=50_000_000),
            name="block",
        )(residual, gain_mlp.reshape(1, width), gain_attn.reshape(1, width), w_gate.T, w_up.T, w_down, w_qkv)
        return pl.pallas_call(
            last_kernel,
            out_shape=(jax.ShapeDtypeStruct((tokens, width), BF16), jax.ShapeDtypeStruct((tokens, qkv), BF16)),
            in_specs=[vmem_spec] * 4,
            out_specs=(any_spec,) * 2,
            scratch_shapes=[pltpu.VMEM((tokens - CUT * CHUNK, qkv), BF16), pltpu.SemaphoreType.DMA((4,))],
            compiler_params=pltpu.CompilerParams(vmem_limit_bytes=16_000_000),
            name="last",
        )(*(pltpu.with_memory_space_constraint(v, pltpu.VMEM) for v in held))

    return jax.shard_map(
        per_device, mesh=mesh,
        in_specs=(P('data', 'row'), P('row'), P('row'), P(None, ('col', 'row')), P(None, ('col', 'row')),
                  P('col', 'row'), P(None, ('col', 'row'))),
        out_specs=(P('data', 'row'), P('data', ('col', 'row'))), check_vma=False)
```

```python
import functools
import math

import jax
import jax.numpy as jnp
from jax import lax
from jax.experimental import pallas as pl
from jax.experimental.pallas import tpu as pltpu
from jax.sharding import PartitionSpec as P

NORM_EPS = 1e-6
MESH = pl.DeviceIdType.MESH
F32, BF16 = jnp.float32, jnp.bfloat16

SLICE = 128
RELAYED, DIRECT = 3, 5
NEAR = ((0, 352), (352, 336), (688, 352), (1040, 336))
WIDE = ((0, 688), (688, 688))
GROUPS = ((0, 384), (384, 384), (768, 384), (1152, 224))
BESIDE = ((("d", 0, 0),), (("d", 0, 1),), (("d", 1, 0),), (("d", 1, 1), ("d", 2, 0)), (("d", 2, 1), ("r", 0, 0)))
PASSES = (((("d", 0), ("d", 1)), ((("r", 0, 1),), (("r", 1, 0), ("d", 3, None)))),
          ((("d", 2), ("r", 0)), ((("r", 1, 1),), (("d", 4, None), ("r", 2, 0), ("r", 2, 1)))),
          ((("d", 3), ("r", 1)), ((), ())),
          ((("d", 4), ("r", 2)), ()))
CHUNK, CHUNKS = 32, 8
SPLIT_CHUNKS = (0,)
DIAGONAL = "xxxxyxyd"
LATE_PARTS = 1
CUT = 4
STEPS = (
    "fwd0", "dfar0", "dfs0", "fwd1", "dfar1", "dfs1", "fwd2", "dfar2", "dfs2", "comb0", "sy0", "fwd3",
    "dfar3", "dfs3", "comb1", "sy1", "fwd4", "dfar4", "dfs4", "comb2", "sy2", "fwd5", "dfar5", "cy0",
    "dfs5", "comb3", "sy3", "fwd6", "dfar6", "cy1", "dfs6", "fwd7", "comb4", "sy4", "dfar7", "cx0",
    "cy2", "dfs7", "cx1", "cx2", "comb5", "sy5", "cd0", "cy3", "cx3", "fin0", "cd1", "comb6",
    "sy6", "cx4", "cy4", "fin1", "cd2", "cx5", "comb7", "sy7", "fin2", "cd3", "cy5", "cx6",
    "cy6", "fin3", "cd4", "proj0", "proj1", "cy7", "cx7", "fin4", "cd5", "cd6", "cd7", "proj2",
    "fin5", "fins6",
)
W_PARTS = 8


def dot(a, b):
    return jnp.dot(a, b, preferred_element_type=F32)


def dot_t(a, b):
    return lax.dot_general(a, b, (((1,), (1,)), ((), ())), preferred_element_type=F32)


def scoped(fn):
    @functools.wraps(fn)
    def run(*args):
        with jax.named_scope("#".join([fn.__name__] + [str(a) for a in args])):
            return fn(*args)
    return run


class Names:
    def __init__(self):
        self.table = {}

    def __call__(self, *key):
        return self.table.setdefault(earlier(key), len(self.table))


def earlier(key):
    if key[0] != "xn":
        return key
    tag, t = key[1:]
    if tag == "x":
        return ("xx",) + ((t // 2, t % 2) if t < 2 * RELAYED else (t - RELAYED, None))
    if tag == "y":
        return ("xy", t // 2, t % 2) if t < 2 * RELAYED else ("rs", t - 2 * RELAYED, 0)
    if tag == "s":
        return ("as",) if t == 0 else ("af", t - 1)
    return ("xf", t) if t < len(PASSES) else (("sq",), ("xs",), ("gs",), ("g1",))[t - len(PASSES)]


def kernel(tokens, width, ff, names, local_names,
           x_hbm, g1_hbm, g2_hbm, wg_hbm, wu_hbm, wd_hbm, wq_hbm, res, out, nb, wq,
           xg, wg, wu, wd, ag, acc, rbuf, xn, gains, sq, scale, gacc, uacc, send_sem, recv_sem, loc_sem):
    data, y, row = lax.axis_index("data"), lax.axis_index("col"), lax.axis_index("row")
    cx = row // 2
    core = row - cx * 2
    sib_row = cx * 2 + 1 - core
    far_row = (1 - cx) * 2 + core
    fsib_row = (1 - cx) * 2 + 1 - core
    sib, far, fsib = (data, y, sib_row), (data, y, far_row), (data, y, fsib_row)
    up, diag = (data, 1 - y, row), (data, 1 - y, far_row)
    hidden = width * 4
    wide = ag.shape[2]
    slices = width // SLICE

    def remote(key, src, dst, dev):
        return pltpu.make_async_remote_copy(src_ref=src, dst_ref=dst, send_sem=send_sem.at[1 if key[0] == "sq" else 0], recv_sem=recv_sem.at[names(*key)],
                                            device_id=dev, device_id_type=MESH)

    def local(key, src, dst):
        return pltpu.make_async_copy(src, dst, loc_sem.at[local_names(*key)])

    def arrived(key, like):
        pltpu.make_async_copy(like, like, recv_sem.at[names(*key)]).wait()

    def loaded(key, like):
        pltpu.make_async_copy(like, like, loc_sem.at[local_names(*key)]).wait()

    sent = []

    def go(key, ref, dev, dst=None):
        copy = remote(key, ref, ref if dst is None else dst, dev)
        copy.start()
        if key[0] != "sq":
            sent.append(math.prod(ref.shape) * jnp.dtype(ref.dtype).itemsize)
        return copy

    own = [local(("x",), x_hbm, xg.at[row]), local(("g1",), g1_hbm, gains.at[row, 0]), local(("g2",), g2_hbm, gains.at[row, 1])]
    for c in own:
        c.start()
    near = pl.ds(pl.multiple_of(cx * 2 * width, 2 * width), 2 * width)
    away = pl.ds(pl.multiple_of((1 - cx) * 2 * width, 2 * width), 2 * width)
    for part in (near, away):
        for g, (c0, cn) in enumerate(NEAR):
            for src, dst in ((wg_hbm, wg), (wu_hbm, wu)):
                key = ("w", g) if part is near else ("w", len(NEAR))
                local(key, src.at[pl.ds(c0, cn), part], dst.at[pl.ds(c0, cn), part]).start()
    for i in range(4):
        local(("wd",), wd_hbm.at[pl.ds(i * ff, ff)], wd.at[i]).start()
    part = hidden // W_PARTS
    for i in range(W_PARTS):
        local(("wq",), wq_hbm.at[pl.ds(i * part, part)], wq.at[pl.ds(i * part, part)]).start()

    barrier = pltpu.get_barrier_semaphore()
    for dev in (sib, far, fsib, up, diag):
        pl.semaphore_signal(barrier, inc=1, device_id=dev, device_id_type=MESH)

    with jax.named_scope("own"):
        if wide > ff:
            ag[row, :, ff:] = jnp.zeros((tokens, wide - ff), BF16)
        for c in own:
            c.wait()
        part = sum(jnp.square(xg[row, :, i:i + 128].astype(F32)) for i in range(0, width, 128)).T
        sq[row] = jnp.sum(part, axis=0, keepdims=True)
    with jax.named_scope("barrier"):
        pl.semaphore_wait(barrier, 5)

    def cut(k):
        return pl.ds(pl.multiple_of(k * SLICE, SLICE), SLICE)

    def direct_slice(p):
        return y * (slices - RELAYED) + p if p < RELAYED else p

    def relayed_slice(q):
        return (1 - y) * (slices - RELAYED) + q

    def slice_of(item):
        return direct_slice(item[1]) if item[0] == "d" else relayed_slice(item[1])

    def parts(item):
        return (0, 1) if item[0] == "r" or item[1] < RELAYED else (None,)

    def x_block(b, item):
        toks = slice(None) if item[2] is None else pl.ds(item[2] * (tokens // 2), tokens // 2)
        return xg.at[b, toks, cut(slice_of(item))]

    x_in = {}
    pass_of = {item: i for i, (items, _) in enumerate(PASSES) for item in items}

    def send_x(p):
        for h in parts(("d", p)):
            x_in["d", p, h] = go(("xx", p, h), x_block(row, ("d", p, h)), far)

    for dev in (far, fsib, sib):
        go(("sq",), sq.at[row], dev)
    x_sib = go(("xs",), xg.at[row], sib)
    go(("gs",), gains.at[row], sib)
    send_x(0)
    for dev in (far, fsib):
        go(("g1",), gains.at[row, 0], dev)
    for p in range(1, DIRECT):
        send_x(p)
    for dev in (far, fsib):
        go(("g2",), gains.at[row, 1], dev)

    def norm_slice(b, k):
        cols = pl.ds(pl.multiple_of(b * width + k * SLICE, SLICE), SLICE)
        nb[:, cols] = (xg[b, :, cut(k)].astype(F32) * scale[...] * gains[b, 0, :, cut(k)]).astype(BF16)

    def norm_block(b):
        def step(k, carry):
            norm_slice(b, k)
            return carry
        lax.fori_loop(0, slices, step, 0)

    @scoped
    def relay(*item):
        x_in[item].wait_recv()
        blk = x_block(far_row, item)
        kind, p, h = item
        if kind == "d" and p < RELAYED:
            x_in["r", p, h] = go(("xy", p, h), blk, up)
        go(("xf", pass_of[kind, p]), blk, sib)

    with jax.named_scope("stats"):
        arrived(("sq",), sq.at[pl.ds(0, 3)])
        mean = (sq[0] + sq[1] + sq[2] + sq[3]) / hidden
        scale[...] = jnp.broadcast_to(lax.rsqrt(mean + NORM_EPS), (128, tokens)).T
    with jax.named_scope("norm_own"):
        norm_block(row)
    with jax.named_scope("norm_sib"):
        x_sib.wait_recv()
        arrived(("gs",), gains.at[0])
        norm_block(sib_row)

    for item in BESIDE[0]:
        relay(*item)
    for g, (c0, cn) in enumerate(NEAR):
        cols = slice(c0, c0 + cn)
        with jax.named_scope(f"gu_near#{g}"):
            loaded(("w", g), wg.at[pl.ds(0, cn)])
            gacc[cols] = dot_t(wg[cols, near], nb[:, near])
            uacc[cols] = dot_t(wu[cols, near], nb[:, near])
        for item in BESIDE[1 + g]:
            relay(*item)
    arrived(("g1",), gains.at[0])
    loaded(("w", len(NEAR)), wg)

    def send_a(t, c0, cn):
        go(("ax", t), ag.at[row, pl.ds(t * CHUNK, CHUNK), pl.ds(c0, cn)], far)

    for i, (items, relays) in enumerate(PASSES):
        with jax.named_scope(f"norm_pass#{i}"):
            for item in items:
                norm_slice(far_row, slice_of(item))
            arrived(("xf", i), xg.at[0, :, pl.ds(0, len(items) * SLICE)])
            for item in items:
                norm_slice(fsib_row, slice_of(item))
        where = [pl.ds(pl.multiple_of(b * width + slice_of(item) * SLICE, SLICE), SLICE)
                 for item in items for b in (far_row, fsib_row)]

        def product(w, cols):
            return dot_t(jnp.concatenate([w[cols, k] for k in where], axis=1), jnp.concatenate([nb[:, k] for k in where], axis=1))

        if i < len(PASSES) - 1:
            for g, (c0, cn) in enumerate(WIDE if any(relays) else ((0, ff),)):
                cols = slice(c0, c0 + cn)
                with jax.named_scope(f"gu_pass#{i}#{g}"):
                    gate, upv = product(wg, cols), product(wu, cols)
                    gacc[cols] += gate
                    uacc[cols] += upv
                for item in relays[g]:
                    relay(*item)
            continue
        for g, (c0, cn) in enumerate(GROUPS):
            with jax.named_scope(f"gu_last#{g}"):
                cols = slice(c0, c0 + cn)
                gate = gacc[cols] + product(wg, cols)
                upv = uacc[cols] + product(wu, cols)
                ag[row, :, cols] = (jax.nn.silu(gate) * upv).astype(BF16).T
            sent_cn = cn if c0 + cn < ff else wide - c0
            for t in SPLIT_CHUNKS:
                send_a(t, c0, sent_cn)
            go(("as",), ag.at[row, :, pl.ds(c0, sent_cn)], sib)
    for t in range(CHUNKS):
        if t not in SPLIT_CHUNKS:
            send_a(t, 0, wide)

    @scoped
    def forward(t):
        blk = ag.at[far_row, pl.ds(t * CHUNK, CHUNK)]
        arrived(("ax", t), blk)
        go(("af", t), blk, sib)

    loaded(("wd",), wd)
    with jax.named_scope("down_own"):
        acc[...] = dot(ag[row, :, :ff], wd[row])
    with jax.named_scope("down_sib"):
        arrived(("as",), ag.at[sib_row])
        acc[...] += dot(ag[sib_row, :, :ff], wd[sib_row])

    def halves(t):
        t0, tn = t * CHUNK, CHUNK
        hn = tn // 2
        return (pl.ds(pl.multiple_of(t0 + y * hn, hn), hn), pl.ds(pl.multiple_of(t0 + (1 - y) * hn, hn), hn),
                pl.ds(t0 // 2, hn))

    @scoped
    def down_far(t):
        rows = slice(t * CHUNK, (t + 1) * CHUNK)
        acc[rows] += dot(ag[far_row, rows, :ff], wd[far_row])

    def column_parts(t):
        n = LATE_PARTS if t == CHUNKS - 1 else 1
        return [pl.ds(i * (width // n), width // n) for i in range(n)]

    @scoped
    def down_fsib(t):
        rows = slice(t * CHUNK, (t + 1) * CHUNK)
        arrived(("af", t), ag.at[fsib_row, pl.ds(t * CHUNK, CHUNK)])
        _, other, packed = halves(t)
        for i, cols in enumerate(column_parts(t)):
            acc[rows, cols] += dot(ag[fsib_row, rows, :ff], wd[fsib_row, :, cols])
            go(("rs", t, i), acc.at[other, cols], up, rbuf.at[packed, cols])

    @scoped
    def combine(t):
        mine, _, packed = halves(t)
        for i, cols in enumerate(column_parts(t)):
            arrived(("rs", t, i), rbuf.at[packed, cols])
            xn[row, mine, cols] = (xg[row, mine, cols].astype(F32) + (acc[mine, cols] + rbuf[packed, cols])).astype(BF16)
            blk = xn.at[row, mine, cols]
            targets = ([("d", diag)] if DIAGONAL[t] == "d" else []) + [("x", far), ("s", sib)]
            for tag, dev in targets:
                go(("xn", tag, t), blk, dev)

    @scoped
    def send_up(t):
        mine, _, _ = halves(t)
        go(("xn", "y", t), xn.at[row, mine], up)

    @scoped
    def collect(tag, t):
        mine, other, _ = halves(t)
        r, rows = {"y": (row, other), "x": (far_row, mine), "d": (far_row, other)}[tag]
        blk = xn.at[r, rows]
        arrived(("xn", tag, t), blk)
        if (tag, DIAGONAL[t]) in (("y", "x"), ("x", "y")):
            go(("xn", "d", t), blk, far if tag == "y" else up)
        go(("xn", "s", t), blk, sib)

    @scoped
    def finish(t, n=1):
        t0, tn = t * CHUNK, n * CHUNK
        for u in range(t, t + n):
            arrived(("xn", "s", u), xn.at[0, pl.ds(0, 2 * CHUNK)])
        res[pl.ds(t0, tn)] = xn[row, pl.ds(t0, tn)]

        def step(i, carry):
            rows = pl.ds(pl.multiple_of(t0 + i * 16, 16), 16)
            blocks = [xn[b, rows].astype(F32) for b in range(4)]
            total = sum(jnp.sum(v * v, axis=1, keepdims=True) for v in blocks)
            r = lax.rsqrt(total / hidden + NORM_EPS)
            for b in range(4):
                nb[rows, b * width:(b + 1) * width] = (blocks[b] * r * gains[b, 1]).astype(BF16)
            return carry
        lax.fori_loop(0, tn // 16, step, 0, unroll=True)

    @scoped
    def project(i):
        if i == 0:
            loaded(("wq",), wq)
        part = wq.shape[1] // 3
        cols = slice(i * part, (i + 1) * part)
        out[:, cols] = dot(nb[:CUT * CHUNK], wq[:, cols]).astype(BF16)

    arrived(("g2",), gains.at[0])
    steps = {"fwd": forward, "dfar": down_far, "dfs": down_fsib, "comb": combine, "sy": send_up, "cy": functools.partial(collect, "y"),
             "cx": functools.partial(collect, "x"), "cd": functools.partial(collect, "d"), "fin": finish, "fins": lambda t: finish(t, 2), "proj": project}
    for name in STEPS:
        steps[name[:-1]](int(name[-1]))
    with jax.named_scope("drain"):
        pltpu.make_async_copy(sq.at[pl.ds(0, 3)], sq.at[pl.ds(0, 3)], send_sem.at[1]).wait()
        tiles = sum(sent) // (16 * 128 * 2)
        deep = max(d for d in range(1, ff // 16 + 1) if tiles % d == 0)
        like = wg.at[pl.ds(0, deep * 16), pl.ds(0, tiles // deep * 128)]
        pltpu.make_async_copy(like, like, send_sem.at[0]).wait()


def last_kernel(res, first, nb, wq, res_hbm, qkv_hbm, out, sem):
    t0, part = CUT * CHUNK, wq.shape[1] // 2
    copies = [pltpu.make_async_copy(res, res_hbm, sem.at[0]),
              pltpu.make_async_copy(first, qkv_hbm.at[pl.ds(0, t0)], sem.at[1])]
    for c in copies:
        c.start()
    for i in range(2):
        cols = pl.ds(i * part, part)
        out[:, cols] = dot(nb[t0:], wq[:, cols]).astype(BF16)
        c = pltpu.make_async_copy(out.at[:, cols], qkv_hbm.at[pl.ds(t0, out.shape[0]), cols], sem.at[2 + i])
        c.start()
        copies.append(c)
    for c in copies:
        c.wait()


def solution(mesh):
    def per_device(residual, gain_mlp, gain_attn, w_gate, w_up, w_down, w_qkv):
        tokens, width = residual.shape
        ff = w_gate.shape[1]
        qkv = w_qkv.shape[1]
        hidden = width * 4
        any_spec = pl.BlockSpec(memory_space=pl.ANY)
        vmem_spec = pl.BlockSpec(memory_space=pltpu.VMEM)
        held = pl.pallas_call(
            functools.partial(kernel, tokens, width, ff, Names(), Names()),
            out_shape=(pltpu.VMEM((tokens, width), BF16), pltpu.VMEM((CUT * CHUNK, qkv), BF16),
                       pltpu.VMEM((tokens, hidden), BF16), pltpu.VMEM((hidden, qkv), BF16)),
            in_specs=[any_spec] * 7,
            out_specs=(vmem_spec,) * 4,
            scratch_shapes=[
                pltpu.VMEM((4, tokens, width), BF16),
                pltpu.VMEM((ff, hidden), BF16),
                pltpu.VMEM((ff, hidden), BF16),
                pltpu.VMEM((4, ff, width), BF16),
                pltpu.VMEM((4, tokens, (ff + 127) // 128 * 128), BF16),
                pltpu.VMEM((tokens, width), F32),
                pltpu.VMEM((tokens // 2, width), F32),
                pltpu.VMEM((4, tokens, width), BF16),
                pltpu.VMEM((4, 2, 1, width), F32),
                pltpu.VMEM((4, 1, tokens), F32),
                pltpu.VMEM((tokens, 128), F32),
                pltpu.VMEM((ff, tokens), F32),
                pltpu.VMEM((ff, tokens), F32),
                pltpu.SemaphoreType.DMA((2,)),
                pltpu.SemaphoreType.DMA((49,)),
                pltpu.SemaphoreType.DMA((10,)),
            ],
            compiler_params=pltpu.CompilerParams(collective_id=0, has_side_effects=True, vmem_limit_bytes=50_000_000),
            name="block",
        )(residual, gain_mlp.reshape(1, width), gain_attn.reshape(1, width), w_gate.T, w_up.T, w_down, w_qkv)
        return pl.pallas_call(
            last_kernel,
            out_shape=(jax.ShapeDtypeStruct((tokens, width), BF16), jax.ShapeDtypeStruct((tokens, qkv), BF16)),
            in_specs=[vmem_spec] * 4,
            out_specs=(any_spec,) * 2,
            scratch_shapes=[pltpu.VMEM((tokens - CUT * CHUNK, qkv), BF16), pltpu.SemaphoreType.DMA((4,))],
            compiler_params=pltpu.CompilerParams(vmem_limit_bytes=16_000_000),
            name="last",
        )(*(pltpu.with_memory_space_constraint(v, pltpu.VMEM) for v in held))

    return jax.shard_map(
        per_device, mesh=mesh,
        in_specs=(P('data', 'row'), P('row'), P('row'), P(None, ('col', 'row')), P(None, ('col', 'row')),
                  P('col', 'row'), P(None, ('col', 'row'))),
        out_specs=(P('data', 'row'), P('data', ('col', 'row'))), check_vma=False)
```
